256 devices in a mesh: tm: 8 (over y, core), space: 32 (over z, x).
Axes of the slice: x: 4, y: 4, z: 8, core: 2. Of those that a mesh axis runs over, the one named last changes fastest.
Arguments:
- state: bfloat16 [8, 16384, 137], P('tm', 'space'), may hold values from -6 to 6
- obs_start: int32 [131072], P(('tm', 'space')), may hold values from 0 to 16383, as said below
- foot_weight: bfloat16 [131072, 8], P(('tm', 'space')), may hold values from 0.019897461 to 0.29882812
- obs_slot: int32 [131072], P(('tm', 'space')), may hold values from 0 to 6
- obs_frac: float32 [131072], P(('tm', 'space')), may hold values from 0 to 1
- live_count: int32 [8, 32], P('tm', 'space'), may hold values from 64 to 512
- obs_values: float32 [131072, 128], P(('tm', 'space')), may hold values from -6 to 6
- jacobian: bfloat16 [137, 128], replicated, may hold values from -0.5 to 0.5
- inv_var: float32 [128], replicated, may hold values from 0.25 to 4
Outputs:
- departures: float32 [131072, 128], P(('tm', 'space'))
- adjoint: float32 [8, 16384, 137], P('tm', 'space')
The draws below stay inside these ranges and needn't reach their ends.
Inputs may be any that keep to these rules, and one draw needn't show every extreme that they name: `obs_start`: on the devices of space index s, every observation's footprint columns lie within 256 columns of tile s, that is within s * 512 - 256 .. (s + 1) * 512 + 255 taken modulo 16384. `live_count`: rows at or beyond a device's count are padding.
All inputs are finite; a program needn't handle non-finite values.
Results may differ from the reference program's by a relative error of at most 0.008.
Values may be sent and summed in bfloat16 or wider, within the bound.
No kernel may reach another device: no remote copies, remote signals or barrier semaphores. Data moves between devices by JAX's collectives and lax.ppermute only.
A program may use at most 64 MiB of HBM per device.

```python
import math
import jax
import jax.numpy as jnp
from jax import lax

LEV = 137
CHAN = 128
FOOT = 8
COL_DEV = 512
OBS_DEV = 512
HALO = 256
SLOTS = 8
TILES = 32
COLS = 16384
OBS = 131072
N_TM = 8
N_SPACE = 32


def draw_obs_start(key, part):
    total_rows = OBS_DEV * N_TM * N_SPACE
    row_index = jnp.arange(total_rows, dtype=jnp.int32)
    tile_index = row_index // OBS_DEV % N_SPACE
    offset = jax.random.randint(key, (total_rows,), 0, COL_DEV + 2 * HALO - FOOT + 1, dtype=jnp.int32)
    return jnp.mod(tile_index * COL_DEV - HALO + offset, COLS).astype(jnp.int32)


def with_ends(drawn, key, low, top_value):
    longest = drawn.shape.index(max(drawn.shape))
    spots = []
    for shift in (0, 1):
        where = [jax.random.randint(jax.random.fold_in(key, axis), (), 0, length) for axis, length in enumerate(drawn.shape)]
        where[longest] = (where[longest] + shift) % drawn.shape[longest]
        spots.append(tuple(where))
    return drawn.at[spots[0]].set(low).at[spots[1]].set(top_value)


def block_scale(key, extent, split, smallest, largest):
    factor_of = 1.0
    for position, parts in split:
        steps = jax.random.uniform(jax.random.fold_in(jax.random.fold_in(key, 6), position), (parts,), jnp.float32, smallest / len(split), largest / len(split))
        factor_of = factor_of * jnp.repeat(jnp.exp(steps), extent[position] // parts).reshape((-1,) + (1,) * (len(extent) - 1 - position))
    return factor_of


def centred(rng, dims, scale, most, split=(), held_as=jnp.bfloat16):
    array = scale * jax.random.normal(rng, dims, jnp.float32)
    if split:
        array = array * block_scale(rng, dims, split, -0.22, 0.18)
    return jnp.clip(array, -most, most).astype(held_as)


def setup_inputs(seed: int = 0) -> dict:
    streams_of = jax.random.split(jax.random.key(seed), 10)
    state = centred(streams_of[0], (SLOTS, COLS, LEV), 1.0, 6.0, ((0, 8), (1, 32)))
    obs_start = draw_obs_start(jax.random.fold_in(streams_of[9], 71), 0)
    foot_weight = jnp.clip(jnp.exp(math.log(0.29882812) - 2.7092764 * jax.random.uniform(streams_of[2], (OBS, FOOT), jnp.float32) ** block_scale(streams_of[2], (OBS, FOOT), ((0, 256),), -0.2, 0.2)), 0.019897461, 0.29882812).astype(jnp.bfloat16)
    obs_slot = with_ends(jax.random.randint(streams_of[3], (OBS,), 0, SLOTS - 1), jax.random.fold_in(streams_of[3], 1), 0, (SLOTS - 1) - 1).astype(jnp.int32)
    obs_frac = jnp.clip(1.0 * jax.random.uniform(streams_of[4], (OBS,), jnp.float32) ** block_scale(streams_of[4], (OBS,), ((0, 256),), -0.2, 0.2), 0.0, 1.0)
    live_count = with_ends(jax.random.randint(streams_of[5], (SLOTS, TILES), OBS_DEV // 8, OBS_DEV + 1), jax.random.fold_in(streams_of[5], 1), OBS_DEV // 8, OBS_DEV).astype(jnp.int32)
    obs_values = centred(streams_of[6], (OBS, CHAN), 1.0, 6.0, ((0, 256),), jnp.float32)
    jacobian = centred(streams_of[7], (LEV, CHAN), LEV ** -0.5, 0.5)
    inv_var = jnp.clip(jnp.exp(jax.random.uniform(streams_of[8], (CHAN,), jnp.float32, math.log(0.25), math.log(4.0))), 0.25, 4.0)
    return {"state": state, "obs_start": obs_start, "foot_weight": foot_weight, "obs_slot": obs_slot, "obs_frac": obs_frac, "live_count": live_count, "obs_values": obs_values, "jacobian": jacobian, "inv_var": inv_var}


def reference(state, obs_start, foot_weight, obs_slot, obs_frac, live_count, obs_values, jacobian, inv_var):
    cols = state.shape[1]
    groups = live_count.shape[0] * live_count.shape[1]
    per_group = obs_start.shape[0] // groups
    offsets = jnp.arange(FOOT, dtype=jnp.int32)

    def visit(adjoint, inputs):
        start, weight, slot, frac, count, values = inputs
        columns = jnp.mod(start[:, None] + offsets[None, :], cols).astype(jnp.int32)
        lower_slot = slot[:, None].astype(jnp.int32)
        upper_slot = (slot[:, None] + 1).astype(jnp.int32)
        lower = state[lower_slot, columns].astype(jnp.float32)
        upper = state[upper_slot, columns].astype(jnp.float32)
        weight_f = weight.astype(jnp.float32)
        p_lower = jnp.einsum("rk,rkl->rl", weight_f, lower, precision=lax.Precision.HIGHEST)
        p_upper = jnp.einsum("rk,rkl->rl", weight_f, upper, precision=lax.Precision.HIGHEST)
        interp = (1.0 - frac)[:, None] * p_lower + frac[:, None] * p_upper
        projected = jnp.dot(interp.astype(jnp.bfloat16), jacobian, preferred_element_type=jnp.float32)
        live = jnp.arange(per_group, dtype=jnp.int32) < count
        departures = jnp.where(live[:, None], values - projected, jnp.float32(0.0))
        scaled = (departures * inv_var[None, :]).astype(jnp.bfloat16)
        back = jnp.dot(scaled, jnp.transpose(jacobian), preferred_element_type=jnp.float32).astype(jnp.bfloat16)
        back = lax.optimization_barrier(back).astype(jnp.float32)
        v_lower = ((1.0 - frac)[:, None] * back).astype(jnp.bfloat16)
        v_upper = (frac[:, None] * back).astype(jnp.bfloat16)
        v_lower = lax.optimization_barrier(v_lower).astype(jnp.float32)
        v_upper = lax.optimization_barrier(v_upper).astype(jnp.float32)
        adjoint = adjoint.at[lower_slot, columns].add(weight_f[:, :, None] * v_lower[:, None, :])
        adjoint = adjoint.at[upper_slot, columns].add(weight_f[:, :, None] * v_upper[:, None, :])
        return adjoint, departures

    inputs = (
        obs_start.reshape(groups, per_group),
        foot_weight.reshape(groups, per_group, FOOT),
        obs_slot.reshape(groups, per_group),
        obs_frac.reshape(groups, per_group),
        live_count.reshape(groups).astype(jnp.int32),
        obs_values.reshape(groups, per_group, obs_values.shape[1]),
    )
    adjoint, departures = lax.scan(visit, jnp.zeros(state.shape, jnp.float32), inputs)
    return departures.reshape(obs_values.shape), adjoint
```

```python
import functools

import jax
import jax.numpy as jnp
from jax import lax
from jax.experimental import pallas as pl
from jax.experimental.pallas import tpu as pltpu
from jax.sharding import PartitionSpec as P


F32 = jnp.float32
BF16 = jnp.bfloat16
GROUP = 16


def vmem_specs(count):
    return [pl.BlockSpec(memory_space=pltpu.VMEM)] * count


def project_kernel(state, jac, start, weight, slot, frac, base, full, head, tail, info):
    half = full.shape[1] // 2
    field = lax.dot_general(
        jac[...], state[...], (((0,), (1,)), ((), ())), preferred_element_type=F32
    ).astype(BF16)
    full[...] = field
    head[...] = field[:, :half]
    tail[...] = field[:, half:]
    total = base[1]
    local = start[...] - base[0]
    local = jnp.where(local < 0, local + total, local)
    local = jnp.where(local >= total, local - total, local)
    rows = lax.broadcasted_iota(jnp.int32, (8, local.shape[1]), 0)
    extra = jnp.where(rows == 0, local.astype(F32), 0.0)
    extra = jnp.where(rows == 1, slot[...].astype(F32), extra)
    extra = jnp.where(rows == 2, frac[...], extra)
    info[0:8, :] = jnp.transpose(weight[...].astype(F32))
    info[8:16, :] = extra


def footprint(info, mat):
    width, obs = mat.shape
    local = info[8:9, :].astype(jnp.int32)
    low = local & (GROUP - 1)
    high = lax.shift_right_logical(local, 4)
    rows = lax.broadcasted_iota(jnp.int32, (GROUP, obs), 0)
    offset = (rows - low) & (GROUP - 1)
    piece = jnp.zeros((GROUP, obs), F32)
    for k in range(8):
        piece = piece + jnp.where(offset == k, info[k : k + 1, :], 0.0)
    piece = piece.astype(BF16)
    group = (high + jnp.where(rows < low, 1, 0)).astype(F32).astype(BF16)
    zero = jnp.zeros((GROUP, obs), BF16)
    for g in range(width // GROUP):
        mat[g * GROUP : (g + 1) * GROUP, :] = jnp.where(
            group == jnp.full((GROUP, obs), g, BF16), piece, zero
        )


def slot_weight(info, held):
    slot = info[9:10, :]
    frac = info[10:11, :]
    return jnp.where(slot == held, 1.0 - frac, 0.0) + jnp.where(slot + 1.0 == held, frac, 0.0)


def gather_kernel(n, held, *refs):
    infos, pieces = refs[:n], refs[n : n + 6]
    outs = refs[n + 6 : n + 6 + n]
    mat, field = refs[n + 6 + n :]
    chan, cols = pieces[0].shape
    half = cols // 2
    for side in range(2):
        rows = slice(side * chan, (side + 1) * chan)
        mid, left, right = pieces[3 * side : 3 * side + 3]
        field[rows, :half] = left[...]
        field[rows, half : half + cols] = mid[...]
        field[rows, half + cols :] = right[...]
    for j in range(n):
        footprint(infos[j], mat)
        both = jnp.dot(field[...], mat[...], preferred_element_type=F32)
        mine = slot_weight(infos[j], held[0].astype(F32))
        other = slot_weight(infos[j], held[1].astype(F32))
        outs[j][...] = (mine * both[:chan] + other * both[chan:]).astype(BF16)


def depart_kernel(n, count, *refs):
    parts = refs[:n]
    values, inv_var, departures, scaled = refs[n:]
    chan, obs = parts[0].shape
    total = parts[0][...].astype(F32)
    for part in parts[1:]:
        total = total + part[...].astype(F32)
    live = lax.broadcasted_iota(jnp.int32, (obs, chan), 0) < count[0]
    gap = jnp.where(live, values[...] - jnp.transpose(total), 0.0)
    departures[...] = gap
    scaled[...] = jnp.transpose(gap * inv_var[...]).astype(BF16)


def spread_kernel(n, held, *refs):
    infos, scaled = refs[:n], refs[n : 2 * n]
    own, give, own_left, own_right, give_left, give_right = refs[2 * n : 2 * n + 6]
    mat, acc = refs[2 * n + 6 :]
    chan = scaled[0].shape[0]
    cols = own.shape[1]
    half = cols // 2
    for j in range(n):
        footprint(infos[j], mat)
        source = scaled[j][...].astype(F32)
        mine = (slot_weight(infos[j], held[0].astype(F32)) * source).astype(BF16)
        other = (slot_weight(infos[j], held[1].astype(F32)) * source).astype(BF16)
        part = lax.dot_general(
            jnp.concatenate([mine, other], axis=0),
            mat[...],
            (((1,), (1,)), ((), ())),
            preferred_element_type=F32,
        )
        if j == 0:
            acc[...] = part
        else:
            acc[...] += part
    own[...] = acc[:chan, half : half + cols]
    give[...] = acc[chan:, half : half + cols].astype(BF16)
    own_left[...] = acc[:chan, :half].astype(BF16)
    own_right[...] = acc[:chan, half + cols :].astype(BF16)
    give_left[...] = acc[chan:, :half].astype(BF16)
    give_right[...] = acc[chan:, half + cols :].astype(BF16)


def finish_kernel(own, center, head0, head1, tail0, tail1, jac, out):
    half = head0.shape[1]
    total = own[...] + center[...].astype(F32)
    first = total[:, :half] + head0[...].astype(F32) + head1[...].astype(F32)
    last = total[:, half:] + tail0[...].astype(F32) + tail1[...].astype(F32)
    for index, part in enumerate((first, last)):
        out[index * half : (index + 1) * half, :] = lax.dot_general(
            part.astype(BF16), jac[...], (((0,), (1,)), ((), ())), preferred_element_type=F32
        )


def call(kernel, outs, *args, scalars=0, scratch=(), flops=1 << 20):
    return pl.pallas_call(
        kernel,
        out_shape=[jax.ShapeDtypeStruct(shape, dtype) for shape, dtype in outs],
        in_specs=[pl.BlockSpec(memory_space=pltpu.SMEM)] * scalars + vmem_specs(len(args) - scalars),
        out_specs=vmem_specs(len(outs)),
        scratch_shapes=[pltpu.VMEM(shape, dtype) for shape, dtype in scratch],
        compiler_params=pltpu.CompilerParams(vmem_limit_bytes=32 << 20),
        cost_estimate=pl.CostEstimate(flops=flops, bytes_accessed=1 << 20, transcendentals=0),
    )(*args)


def make_body(n_tm, n_space):
    lanes = n_tm // 2

    def move(block, turn, swap, shift):
        route = []
        for t in range(n_tm):
            for s in range(n_space):
                y, core = t // 2, t % 2
                t_from = ((y + turn) % lanes) * 2 + (core ^ swap)
                s_from = (s + shift) % n_space
                route.append((t_from * n_space + s_from, t * n_space + s))
        return lax.ppermute(block, ("tm", "space"), route)

    def body(
        state, obs_start, foot_weight, obs_slot, obs_frac, live_count, obs_values, jacobian, inv_var
    ):
        own = state[0]
        cols, levels = own.shape
        half = cols // 2
        width = 2 * cols
        chan = jacobian.shape[1]
        obs = obs_start.shape[0]
        tile = lax.axis_index("space")
        turn = lax.axis_index("tm")
        total_cols = cols * n_space
        base = jnp.stack([tile * cols - half, jnp.int32(total_cols)]).astype(jnp.int32)
        held = jnp.stack([turn, turn ^ 1]).astype(jnp.int32)

        def flat(vector):
            return vector.reshape(1, -1)

        full, head, tail, info = pl.pallas_call(
            project_kernel,
            out_shape=[
                jax.ShapeDtypeStruct((chan, cols), BF16),
                jax.ShapeDtypeStruct((chan, half), BF16),
                jax.ShapeDtypeStruct((chan, half), BF16),
                jax.ShapeDtypeStruct((16, obs), F32),
            ],
            in_specs=vmem_specs(6) + [pl.BlockSpec(memory_space=pltpu.SMEM)],
            out_specs=vmem_specs(4),
            compiler_params=pltpu.CompilerParams(vmem_limit_bytes=32 << 20),
        )(own, jacobian, flat(obs_start), foot_weight, flat(obs_slot), flat(obs_frac), base)

        infos = [info] + [move(info, j, 0, 0) for j in range(1, lanes)]
        pieces = [
            full,
            move(tail, 0, 0, -1),
            move(head, 0, 0, 1),
            move(full, 0, 1, 0),
            move(tail, 0, 1, -1),
            move(head, 0, 1, 1),
        ]
        parts = call(
            functools.partial(gather_kernel, lanes),
            [((chan, obs), BF16)] * lanes,
            held,
            *infos,
            *pieces,
            scalars=1,
            scratch=[((width, obs), BF16), ((2 * chan, width), BF16)],
        )
        parts = [parts[0]] + [move(parts[j], -j, 0, 0) for j in range(1, lanes)]
        departures, scaled = call(
            functools.partial(depart_kernel, lanes),
            [((obs, chan), F32), ((chan, obs), BF16)],
            live_count.reshape(1),
            *parts,
            obs_values,
            flat(inv_var),
            scalars=1,
        )
        all_scaled = [scaled] + [move(scaled, j, 0, 0) for j in range(1, lanes)]
        mine, give, own_left, own_right, give_left, give_right = call(
            functools.partial(spread_kernel, lanes),
            [((chan, cols), F32), ((chan, cols), BF16)] + [((chan, half), BF16)] * 4,
            held,
            *infos,
            *all_scaled,
            scalars=1,
            scratch=[((width, obs), BF16), ((2 * chan, width), F32)],
        )
        (adjoint,) = call(
            finish_kernel,
            [((cols, levels), F32)],
            mine,
            move(give, 0, 1, 0),
            move(own_right, 0, 0, -1),
            move(give_right, 0, 1, -1),
            move(own_left, 0, 0, 1),
            move(give_left, 0, 1, 1),
            jacobian,
        )
        return (departures, adjoint[None])

    return body


def solution(mesh):
    return jax.shard_map(
        make_body(mesh.shape["tm"], mesh.shape["space"]),
        mesh=mesh,
        in_specs=(
            P("tm", "space", None),
            P(("tm", "space")),
            P(("tm", "space"), None),
            P(("tm", "space")),
            P(("tm", "space")),
            P("tm", "space"),
            P(("tm", "space"), None),
            P(),
            P(),
        ),
        out_specs=(P(("tm", "space"), None), P("tm", "space", None)),
        check_vma=False,
    )
```

```python
import functools

import jax
import jax.numpy as jnp
from jax import lax
from jax.experimental import pallas as pl
from jax.experimental.pallas import tpu as pltpu
from jax.sharding import PartitionSpec as P


F32 = jnp.float32
BF16 = jnp.bfloat16
GROUP = 16


def vmem_specs(count):
    return [pl.BlockSpec(memory_space=pltpu.VMEM)] * count


def project_kernel(state, jac, start, weight, slot, frac, base, full, head, tail, info):
    half = full.shape[1] // 2
    field = lax.dot_general(
        jac[...], state[...], (((0,), (0,)), ((), ())), preferred_element_type=F32
    ).astype(BF16)
    full[...] = field
    head[...] = field[:, :half]
    tail[...] = field[:, half:]
    total = base[1]
    local = start[...] - base[0]
    local = jnp.where(local < 0, local + total, local)
    local = jnp.where(local >= total, local - total, local)
    rows = lax.broadcasted_iota(jnp.int32, (8, local.shape[1]), 0)
    extra = jnp.where(rows == 0, local.astype(F32), 0.0)
    extra = jnp.where(rows == 1, slot[...].astype(F32), extra)
    extra = jnp.where(rows == 2, frac[...], extra)
    info[0:8, :] = weight[...].astype(F32)
    info[8:16, :] = extra


def widen_kernel(full, left, right, wide):
    cols = full.shape[1]
    half = cols // 2
    wide[:, :half] = left[...]
    wide[:, half : half + cols] = full[...]
    wide[:, half + cols :] = right[...]


def matrix_kernel(n, *refs):
    for info, mat in zip(refs[:n], refs[n:]):
        footprint(info, mat)


def footprint(info, mat):
    width, obs = mat.shape
    local = info[8:9, :].astype(jnp.int32)
    low = local & (GROUP - 1)
    high = lax.shift_right_logical(local, 4)
    rows = lax.broadcasted_iota(jnp.int32, (GROUP, obs), 0)
    offset = (rows - low) & (GROUP - 1)
    piece = jnp.zeros((GROUP, obs), F32)
    for k in range(8):
        piece = piece + jnp.where(offset == k, info[k : k + 1, :], 0.0)
    piece = piece.astype(BF16)
    group = (high + jnp.where(rows < low, 1, 0)).astype(F32).astype(BF16)
    zero = jnp.zeros((GROUP, obs), BF16)
    for g in range(width // GROUP):
        mat[g * GROUP : (g + 1) * GROUP, :] = jnp.where(
            group == jnp.full((GROUP, obs), g, BF16), piece, zero
        )


def slot_weight(info, held):
    slot = info[9:10, :]
    frac = info[10:11, :]
    return jnp.where(slot == held, 1.0 - frac, 0.0) + jnp.where(slot + 1.0 == held, frac, 0.0)


def gather_kernel(n, held, mine, other, *refs):
    infos, mats, outs = refs[:n], refs[n : 2 * n], refs[2 * n :]
    chan = mine.shape[0]
    field = jnp.concatenate([mine[...], other[...]], axis=0)
    for info, mat, out in zip(infos, mats, outs):
        both = jnp.dot(field, mat[...], preferred_element_type=F32)
        first = slot_weight(info, held[0].astype(F32))
        second = slot_weight(info, held[1].astype(F32))
        out[...] = (first * both[:chan] + second * both[chan:]).astype(BF16)


def turn_kernel(source, out):
    out[...] = jnp.transpose(source[...])


def depart_kernel(n, count, *refs):
    parts = refs[:n]
    values, inv_var, gaps, scaled = refs[n:]
    chan, obs = values.shape
    total = parts[0][...].astype(F32)
    for part in parts[1:]:
        total = total + part[...].astype(F32)
    live = lax.broadcasted_iota(jnp.int32, (chan, obs), 1) < count[0]
    gap = jnp.where(live, values[...] - total, 0.0)
    gaps[...] = gap
    scaled[...] = (gap * inv_var[...]).astype(BF16)


def spread_part(held, infos, scaled, mats):
    total = None
    for info, source, mat in zip(infos, scaled, mats):
        rows = source[...].astype(F32)
        mine = (slot_weight(info, held[0].astype(F32)) * rows).astype(BF16)
        other = (slot_weight(info, held[1].astype(F32)) * rows).astype(BF16)
        part = lax.dot_general(
            jnp.concatenate([mine, other], axis=0),
            mat[...],
            (((1,), (1,)), ((), ())),
            preferred_element_type=F32,
        )
        total = part if total is None else total + part
    return total


def spread_own_kernel(held, info, scaled, mat, acc):
    acc[...] = spread_part(held, [info], [scaled], [mat])


def spread_rest_kernel(n, held, acc, *refs):
    infos, scaled, mats = refs[:n], refs[n : 2 * n], refs[2 * n : 3 * n]
    own, give = refs[3 * n :]
    chan = own.shape[0]
    total = acc[...] + spread_part(held, infos, scaled, mats)
    own[...] = total[:chan]
    give[...] = total[chan:].astype(BF16)


def join_kernel(own, got, mid, left, right):
    cols = mid.shape[1]
    half = cols // 2
    mid[...] = own[:, half : half + cols] + got[:, half : half + cols].astype(F32)
    left[...] = (own[:, :half] + got[:, :half].astype(F32)).astype(BF16)
    right[...] = (own[:, half + cols :] + got[:, half + cols :].astype(F32)).astype(BF16)


def finish_kernel(mid, head, tail, jac, out):
    half = head.shape[1]
    first = mid[:, :half] + head[...].astype(F32)
    last = mid[:, half:] + tail[...].astype(F32)
    total = jnp.concatenate([first, last], axis=1).astype(BF16)
    out[:, 0, :] = jnp.dot(jac[...], total, preferred_element_type=F32)


def call(kernel, outs, *args, scalars=0, scratch=(), flops=1 << 20):
    return pl.pallas_call(
        kernel,
        out_shape=[jax.ShapeDtypeStruct(shape, dtype) for shape, dtype in outs],
        in_specs=[pl.BlockSpec(memory_space=pltpu.SMEM)] * scalars + vmem_specs(len(args) - scalars),
        out_specs=vmem_specs(len(outs)),
        scratch_shapes=[pltpu.VMEM(shape, dtype) for shape, dtype in scratch],
        compiler_params=pltpu.CompilerParams(vmem_limit_bytes=8 << 20),
        cost_estimate=pl.CostEstimate(flops=flops, bytes_accessed=1 << 20, transcendentals=0),
    )(*args)


def make_body(n_tm, n_space):
    lanes = n_tm // 2

    def move(block, turn, swap, shift):
        route = []
        for t in range(n_tm):
            for s in range(n_space):
                y, core = t // 2, t % 2
                t_from = ((y + turn) % lanes) * 2 + (core ^ swap)
                s_from = (s + shift) % n_space
                route.append((t_from * n_space + s_from, t * n_space + s))
        return lax.ppermute(block, ("tm", "space"), route)

    def body(
        state, obs_start, foot_weight, obs_slot, obs_frac, live_count, obs_values, jacobian, inv_var
    ):
        own = state[0]
        cols, levels = own.shape
        half = cols // 2
        width = 2 * cols
        chan = jacobian.shape[1]
        obs = obs_start.shape[0]
        tile = lax.axis_index("space")
        turn = lax.axis_index("tm")
        total_cols = cols * n_space
        base = jnp.stack([tile * cols - half, jnp.int32(total_cols)]).astype(jnp.int32)
        held = jnp.stack([turn, turn ^ 1]).astype(jnp.int32)

        def flat(vector):
            return vector.reshape(1, -1)

        full, head, tail, info = pl.pallas_call(
            project_kernel,
            out_shape=[
                jax.ShapeDtypeStruct((chan, cols), BF16),
                jax.ShapeDtypeStruct((chan, half), BF16),
                jax.ShapeDtypeStruct((chan, half), BF16),
                jax.ShapeDtypeStruct((16, obs), F32),
            ],
            in_specs=vmem_specs(6) + [pl.BlockSpec(memory_space=pltpu.SMEM)],
            out_specs=vmem_specs(4),
            compiler_params=pltpu.CompilerParams(vmem_limit_bytes=8 << 20),
        )(own.T, jacobian, flat(obs_start), foot_weight.T, flat(obs_slot), flat(obs_frac), base)

        left, right = move(tail, 0, 0, -1), move(head, 0, 0, 1)
        infos = [info] + [move(info, j, 0, 0) for j in range(1, lanes)]
        (wide,) = call(widen_kernel, [((chan, width), BF16)], full, left, right)
        other = move(wide, 0, 1, 0)
        mats = call(
            functools.partial(matrix_kernel, lanes), [((width, obs), BF16)] * lanes, *infos
        )

        def gather(which):
            return call(
                functools.partial(gather_kernel, len(which)),
                [((chan, obs), BF16)] * len(which),
                held,
                wide,
                other,
                *[infos[j] for j in which],
                *[mats[j] for j in which],
                scalars=1,
            )

        (far,) = gather([2])
        far = move(far, -2, 0, 0)
        after, before = gather([1, 3])
        after, before = move(after, -1, 0, 0), move(before, 1, 0, 0)
        (kept,) = gather([0])
        (values,) = call(turn_kernel, [((chan, obs), F32)], obs_values)
        gaps, scaled = call(
            functools.partial(depart_kernel, lanes),
            [((chan, obs), F32), ((chan, obs), BF16)],
            live_count.reshape(1),
            kept,
            far,
            after,
            before,
            values,
            inv_var.reshape(-1, 1),
            scalars=1,
        )
        all_scaled = [scaled] + [move(scaled, j, 0, 0) for j in range(1, lanes)]
        (acc,) = call(
            spread_own_kernel,
            [((2 * chan, width), F32)],
            held,
            info,
            scaled,
            mats[0],
            scalars=1,
        )
        (departures,) = call(turn_kernel, [((obs, chan), F32)], gaps)
        mine, give = call(
            functools.partial(spread_rest_kernel, lanes - 1),
            [((chan, width), F32), ((chan, width), BF16)],
            held,
            acc,
            *infos[1:],
            *all_scaled[1:],
            *mats[1:],
            scalars=1,
        )
        mid, to_left, to_right = call(
            join_kernel,
            [((chan, cols), F32)] + [((chan, half), BF16)] * 2,
            mine,
            move(give, 0, 1, 0),
        )
        (adjoint,) = call(
            finish_kernel,
            [((levels, 1, cols), F32)],
            mid,
            move(to_right, 0, 0, -1),
            move(to_left, 0, 0, 1),
            jacobian,
        )
        return (departures, jnp.transpose(adjoint, (1, 2, 0)))

    return body


def solution(mesh):
    return jax.shard_map(
        make_body(mesh.shape["tm"], mesh.shape["space"]),
        mesh=mesh,
        in_specs=(
            P("tm", "space", None),
            P(("tm", "space")),
            P(("tm", "space"), None),
            P(("tm", "space")),
            P(("tm", "space")),
            P("tm", "space"),
            P(("tm", "space"), None),
            P(),
            P(),
        ),
        out_specs=(P(("tm", "space"), None), P("tm", "space", None)),
        check_vma=False,
    )
```

```python
import functools

import jax
import jax.numpy as jnp
from jax import lax
from jax.experimental import pallas as pl
from jax.experimental.pallas import tpu as pltpu
from jax.sharding import PartitionSpec as P


F32 = jnp.float32
BF16 = jnp.bfloat16
GROUP = 16


VMEM = pl.BlockSpec(memory_space=pltpu.VMEM)
SMEM = pl.BlockSpec(memory_space=pltpu.SMEM)
HBM = pl.BlockSpec(memory_space=pltpu.HBM)


def held_slots():
    turn = lax.axis_index("tm")
    return turn.astype(F32), (turn ^ 1).astype(F32)


def project_kernel(state, jac, full, head, tail, field, levels, sems):
    half = full.shape[1] // 2
    copies = [
        pltpu.make_async_copy(state, field, sems.at[0]),
        pltpu.make_async_copy(jac, levels, sems.at[1]),
    ]
    for copy in copies:
        copy.start()
    for copy in copies:
        copy.wait()
    out = lax.dot_general(
        levels[...], field[...], (((0,), (0,)), ((), ())), preferred_element_type=F32
    ).astype(BF16)
    full[...] = out
    head[...] = out[:, :half]
    tail[...] = out[:, half:]


def info_kernel(cols, tiles, start, weight, slot, frac, info):
    base = lax.axis_index("space") * cols - cols // 2
    total = cols * tiles
    local = start[...] - base
    local = jnp.where(local < 0, local + total, local)
    local = jnp.where(local >= total, local - total, local)
    rows = lax.broadcasted_iota(jnp.int32, (8, local.shape[1]), 0)
    extra = jnp.where(rows == 0, local.astype(F32), 0.0)
    extra = jnp.where(rows == 1, slot[...].astype(F32), extra)
    extra = jnp.where(rows == 2, frac[...], extra)
    info[0:8, :] = weight[...].astype(F32)
    info[8:16, :] = extra


def widen_kernel(full, left, right, wide):
    cols = full.shape[1]
    half = cols // 2
    wide[:, :half] = left[...]
    wide[:, half : half + cols] = full[...]
    wide[:, half + cols :] = right[...]


def matrix_kernel(n, *refs):
    for info, mat in zip(refs[:n], refs[n:]):
        footprint(info, mat)


def footprint(info, mat):
    width, obs = mat.shape
    local = info[8:9, :].astype(jnp.int32)
    low = local & (GROUP - 1)
    high = lax.shift_right_logical(local, 4)
    rows = lax.broadcasted_iota(jnp.int32, (GROUP, obs), 0)
    offset = (rows - low) & (GROUP - 1)
    piece = jnp.zeros((GROUP, obs), F32)
    for k in range(8):
        piece = piece + jnp.where(offset == k, info[k : k + 1, :], 0.0)
    piece = piece.astype(BF16)
    group = (high + jnp.where(rows < low, 1, 0)).astype(F32).astype(BF16)
    zero = jnp.zeros((GROUP, obs), BF16)
    for g in range(width // GROUP):
        mat[g * GROUP : (g + 1) * GROUP, :] = jnp.where(
            group == jnp.full((GROUP, obs), g, BF16), piece, zero
        )


def slot_weight(info, held):
    slot = info[9:10, :]
    frac = info[10:11, :]
    return jnp.where(slot == held, 1.0 - frac, 0.0) + jnp.where(slot + 1.0 == held, frac, 0.0)


def gather_kernel(n, mine, other, *refs):
    infos, mats, outs = refs[:n], refs[n : 2 * n], refs[2 * n :]
    chan = mine.shape[0]
    field = jnp.concatenate([mine[...], other[...]], axis=0)
    own_slot, other_slot = held_slots()
    for info, mat, out in zip(infos, mats, outs):
        both = jnp.dot(field, mat[...], preferred_element_type=F32)
        first = slot_weight(info, own_slot)
        second = slot_weight(info, other_slot)
        out[...] = (first * both[:chan] + second * both[chan:]).astype(BF16)


def turn_kernel(source, out):
    out[...] = jnp.transpose(source[...])


def values_kernel(source, inv_var, values, scale, held, sem):
    copy = pltpu.make_async_copy(source, held, sem)
    copy.start()
    scale[...] = jnp.transpose(jnp.broadcast_to(inv_var[...], scale.shape))
    copy.wait()
    values[...] = jnp.transpose(held[...])


def depart_kernel(n, count, *refs):
    parts = refs[:n]
    values, scale, gaps, scaled = refs[n:]
    chan, obs = values.shape
    total = parts[0][...].astype(F32)
    for part in parts[1:]:
        total = total + part[...].astype(F32)
    live = lax.broadcasted_iota(jnp.int32, (chan, obs), 1) < count[0, 0]
    gap = jnp.where(live, values[...] - total, 0.0)
    gaps[...] = gap
    scaled[...] = (gap * scale[:, 0:1]).astype(BF16)


def spread_part(infos, scaled, mats):
    own_slot, other_slot = held_slots()
    total = None
    for info, source, mat in zip(infos, scaled, mats):
        rows = source[...].astype(F32)
        mine = (slot_weight(info, own_slot) * rows).astype(BF16)
        other = (slot_weight(info, other_slot) * rows).astype(BF16)
        part = lax.dot_general(
            jnp.concatenate([mine, other], axis=0),
            mat[...],
            (((1,), (1,)), ((), ())),
            preferred_element_type=F32,
        )
        total = part if total is None else total + part
    return total


def spread_own_kernel(info, scaled, mat, acc):
    acc[...] = spread_part([info], [scaled], [mat])


def spread_rest_kernel(n, acc, *refs):
    infos, scaled, mats = refs[:n], refs[n : 2 * n], refs[2 * n : 3 * n]
    own, give = refs[3 * n :]
    chan = own.shape[0]
    total = acc[...] + spread_part(infos, scaled, mats)
    own[...] = total[:chan]
    give[...] = total[chan:].astype(BF16)


def join_kernel(own, got, mid, left, right):
    cols = mid.shape[1]
    half = cols // 2
    mid[...] = own[:, half : half + cols] + got[:, half : half + cols].astype(F32)
    left[...] = (own[:, :half] + got[:, :half].astype(F32)).astype(BF16)
    right[...] = (own[:, half + cols :] + got[:, half + cols :].astype(F32)).astype(BF16)


def finish_kernel(mid, head, tail, jac, out):
    half = head.shape[1]
    first = mid[:, :half] + head[...].astype(F32)
    last = mid[:, half:] + tail[...].astype(F32)
    total = jnp.concatenate([first, last], axis=1).astype(BF16)
    out[:, 0, :] = jnp.dot(jac[...], total, preferred_element_type=F32)


def call(kernel, outs, *args, specs=None, scratch=(), flops=1 << 20):
    return pl.pallas_call(
        kernel,
        out_shape=[jax.ShapeDtypeStruct(shape, dtype) for shape, dtype in outs],
        in_specs=specs or [VMEM] * len(args),
        out_specs=[VMEM] * len(outs),
        scratch_shapes=scratch,
        compiler_params=pltpu.CompilerParams(vmem_limit_bytes=8 << 20),
        cost_estimate=pl.CostEstimate(flops=flops, bytes_accessed=1 << 20, transcendentals=0),
    )(*args)


def make_body(n_tm, n_space):
    lanes = n_tm // 2

    def move(block, turn, swap, shift):
        route = []
        for t in range(n_tm):
            for s in range(n_space):
                y, core = t // 2, t % 2
                t_from = ((y + turn) % lanes) * 2 + (core ^ swap)
                s_from = (s + shift) % n_space
                route.append((t_from * n_space + s_from, t * n_space + s))
        return lax.ppermute(block, ("tm", "space"), route)

    def steps(
        state, obs_start, foot_weight, obs_slot, obs_frac, live_count, obs_values, jacobian, inv_var
    ):
        own = state[0]
        cols, levels = own.shape
        half = cols // 2
        width = 2 * cols
        chan = jacobian.shape[1]
        obs = obs_start.shape[0]

        def flat(vector):
            return vector.reshape(1, -1)

        full, head, tail = call(
            project_kernel,
            [((chan, cols), BF16), ((chan, half), BF16), ((chan, half), BF16)],
            own.T,
            jacobian,
            specs=[HBM, HBM],
            scratch=[
                pltpu.VMEM((levels, cols), BF16),
                pltpu.VMEM((levels, chan), BF16),
                pltpu.SemaphoreType.DMA((2,)),
            ],
        )
        (info,) = call(
            functools.partial(info_kernel, cols, n_space),
            [((16, obs), F32)],
            flat(obs_start),
            foot_weight.T,
            flat(obs_slot),
            flat(obs_frac),
        )
        left, right = move(tail, 0, 0, -1), move(head, 0, 0, 1)
        infos = [info] + [move(info, j, 0, 0) for j in range(1, lanes)]
        (wide,) = call(widen_kernel, [((chan, width), BF16)], full, left, right)
        other = move(wide, 0, 1, 0)
        mats = call(functools.partial(matrix_kernel, lanes), [((width, obs), BF16)] * lanes, *infos)

        def gather(which):
            return call(
                functools.partial(gather_kernel, len(which)),
                [((chan, obs), BF16)] * len(which),
                wide,
                other,
                *[infos[j] for j in which],
                *[mats[j] for j in which],
            )

        (far,) = gather([2])
        far = move(far, -2, 0, 0)
        after, before = gather([1, 3])
        after, before = move(after, -1, 0, 0), move(before, 1, 0, 0)
        (kept,) = gather([0])
        values, scale = call(
            values_kernel,
            [((chan, obs), F32), ((chan, chan), F32)],
            obs_values,
            flat(inv_var),
            specs=[HBM, VMEM],
            scratch=[pltpu.VMEM((obs, chan), F32), pltpu.SemaphoreType.DMA],
        )
        gaps, scaled = call(
            functools.partial(depart_kernel, lanes),
            [((chan, obs), F32), ((chan, obs), BF16)],
            live_count,
            kept,
            far,
            after,
            before,
            values,
            scale,
            specs=[SMEM] + [VMEM] * (lanes + 2),
        )
        all_scaled = [scaled] + [move(scaled, j, 0, 0) for j in range(1, lanes)]
        (acc,) = call(spread_own_kernel, [((2 * chan, width), F32)], info, scaled, mats[0])
        (departures,) = call(turn_kernel, [((obs, chan), F32)], gaps)
        mine, give = call(
            functools.partial(spread_rest_kernel, lanes - 1),
            [((chan, width), F32), ((chan, width), BF16)],
            acc,
            *infos[1:],
            *all_scaled[1:],
            *mats[1:],
        )
        mid, to_left, to_right = call(
            join_kernel,
            [((chan, cols), F32)] + [((chan, half), BF16)] * 2,
            mine,
            move(give, 0, 1, 0),
        )
        (adjoint,) = call(
            finish_kernel,
            [((levels, 1, cols), F32)],
            mid,
            move(to_right, 0, 0, -1),
            move(to_left, 0, 0, 1),
            jacobian,
        )
        return (departures, jnp.transpose(adjoint, (1, 2, 0)))

    return steps


def solution(mesh):
    return jax.shard_map(
        make_body(mesh.shape["tm"], mesh.shape["space"]),
        mesh=mesh,
        in_specs=(
            P("tm", "space", None),
            P(("tm", "space")),
            P(("tm", "space"), None),
            P(("tm", "space")),
            P(("tm", "space")),
            P("tm", "space"),
            P(("tm", "space"), None),
            P(),
            P(),
        ),
        out_specs=(P(("tm", "space"), None), P("tm", "space", None)),
        check_vma=False,
    )
```

```python
import functools

import jax
import jax.numpy as jnp
from jax import lax
from jax.experimental import pallas as pl
from jax.experimental.pallas import tpu as pltpu
from jax.sharding import PartitionSpec as P


F32 = jnp.float32
BF16 = jnp.bfloat16
GROUP = 16


VMEM = pl.BlockSpec(memory_space=pltpu.VMEM)
SMEM = pl.BlockSpec(memory_space=pltpu.SMEM)
HBM = pl.BlockSpec(memory_space=pltpu.HBM)


def held_slots():
    turn = lax.axis_index("tm")
    return turn.astype(F32), (turn ^ 1).astype(F32)


def project_kernel(state, jac, full, head, tail, field, levels, sems):
    half = full.shape[1] // 2
    copies = [
        pltpu.make_async_copy(state, field, sems.at[0]),
        pltpu.make_async_copy(jac, levels, sems.at[1]),
    ]
    for copy in copies:
        copy.start()
    for copy in copies:
        copy.wait()
    out = lax.dot_general(
        levels[...], field[...], (((0,), (0,)), ((), ())), preferred_element_type=F32
    ).astype(BF16)
    full[...] = out
    head[...] = out[:, :half]
    tail[...] = out[:, half:]


def info_kernel(cols, tiles, start, weight, slot, frac, info):
    base = lax.axis_index("space") * cols - cols // 2
    total = cols * tiles
    local = start[...] - base
    local = jnp.where(local < 0, local + total, local)
    local = jnp.where(local >= total, local - total, local)
    rows = lax.broadcasted_iota(jnp.int32, (8, local.shape[1]), 0)
    extra = jnp.where(rows == 0, local.astype(F32), 0.0)
    extra = jnp.where(rows == 1, slot[...].astype(F32), extra)
    extra = jnp.where(rows == 2, frac[...], extra)
    info[0:8, :] = weight[...].astype(F32)
    info[8:16, :] = extra


def widen_kernel(full, left, right, wide):
    cols = full.shape[1]
    half = cols // 2
    wide[:, :half] = left[...]
    wide[:, half : half + cols] = full[...]
    wide[:, half + cols :] = right[...]


def footprint(info, mat):
    width, obs = mat.shape
    local = info[8:9, :].astype(jnp.int32)
    low = local & (GROUP - 1)
    high = lax.shift_right_logical(local, 4)
    rows = lax.broadcasted_iota(jnp.int32, (GROUP, obs), 0)
    offset = (rows - low) & (GROUP - 1)
    piece = jnp.zeros((GROUP, obs), F32)
    for k in range(8):
        piece = piece + jnp.where(offset == k, info[k : k + 1, :], 0.0)
    piece = piece.astype(BF16)
    group = (high + jnp.where(rows < low, 1, 0)).astype(F32).astype(BF16)
    zero = jnp.zeros((GROUP, obs), BF16)
    for g in range(width // GROUP):
        mat[g * GROUP : (g + 1) * GROUP, :] = jnp.where(
            group == jnp.full((GROUP, obs), g, BF16), piece, zero
        )


def slot_weight(info, held):
    slot = info[9:10, :]
    frac = info[10:11, :]
    return jnp.where(slot == held, 1.0 - frac, 0.0) + jnp.where(slot + 1.0 == held, frac, 0.0)


def gather_one(field, info, mat, out):
    chan = out.shape[0]
    own_slot, other_slot = held_slots()
    both = jnp.dot(field, mat[...], preferred_element_type=F32)
    first = slot_weight(info, own_slot)
    second = slot_weight(info, other_slot)
    out[...] = (first * both[:chan] + second * both[chan:]).astype(BF16)


def gather_kernel(mine, other, info, mat, out):
    gather_one(jnp.concatenate([mine[...], other[...]], axis=0), info, mat, out)


def build_gather_kernel(n, mine, other, *refs):
    infos, mats, outs = refs[:n], refs[n : 2 * n], refs[2 * n :]
    field = jnp.concatenate([mine[...], other[...]], axis=0)
    for info, mat, out in zip(infos, mats, outs):
        footprint(info, mat)
        gather_one(field, info, mat, out)


def turn_kernel(source, out):
    out[...] = jnp.transpose(source[...])


def values_kernel(source, inv_var, values, scale, held, sem):
    copy = pltpu.make_async_copy(source, held, sem)
    copy.start()
    scale[...] = jnp.transpose(jnp.broadcast_to(inv_var[...], scale.shape))
    copy.wait()
    values[...] = jnp.transpose(held[...])


def depart_kernel(n, count, *refs):
    parts = refs[:n]
    values, scale, gaps, scaled = refs[n:]
    chan, obs = values.shape
    total = parts[0][...].astype(F32)
    for part in parts[1:]:
        total = total + part[...].astype(F32)
    live = lax.broadcasted_iota(jnp.int32, (chan, obs), 1) < count[0, 0]
    gap = jnp.where(live, values[...] - total, 0.0)
    gaps[...] = gap
    scaled[...] = (gap * scale[:, 0:1]).astype(BF16)


def spread_one(info, source, mat):
    own_slot, other_slot = held_slots()
    rows = source[...].astype(F32)
    mine = (slot_weight(info, own_slot) * rows).astype(BF16)
    other = (slot_weight(info, other_slot) * rows).astype(BF16)
    return lax.dot_general(
        jnp.concatenate([mine, other], axis=0),
        mat[...],
        (((1,), (1,)), ((), ())),
        preferred_element_type=F32,
    )


def spread_first_kernel(info, scaled, mat, acc):
    acc[...] = spread_one(info, scaled, mat)


def spread_next_kernel(before, info, scaled, mat, acc):
    acc[...] = before[...] + spread_one(info, scaled, mat)


def spread_last_kernel(before, info, scaled, mat, own, give):
    chan = own.shape[0]
    total = before[...] + spread_one(info, scaled, mat)
    own[...] = total[:chan]
    give[...] = total[chan:].astype(BF16)


def join_kernel(own, got, mid, left, right):
    cols = mid.shape[1]
    half = cols // 2
    mid[...] = own[:, half : half + cols] + got[:, half : half + cols].astype(F32)
    left[...] = (own[:, :half] + got[:, :half].astype(F32)).astype(BF16)
    right[...] = (own[:, half + cols :] + got[:, half + cols :].astype(F32)).astype(BF16)


def finish_kernel(mid, head, tail, jac, out, rows, sems):
    half = head.shape[1]
    levels = jac.shape[0]
    cut = (levels // 2 + 15) // 16 * 16
    first = mid[:, :half] + head[...].astype(F32)
    last = mid[:, half:] + tail[...].astype(F32)
    total = jnp.concatenate([first, last], axis=1).astype(BF16)
    copies = []
    for index, part in enumerate((slice(0, cut), slice(cut, levels))):
        rows[part, 0, :] = jnp.dot(jac[part, :], total, preferred_element_type=F32)
        copy = pltpu.make_async_copy(rows.at[part], out.at[part], sems.at[index])
        copy.start()
        copies.append(copy)
    for copy in copies:
        copy.wait()


def call(kernel, outs, *args, specs=None, out_specs=None, scratch=(), limit=8 << 20, flops=1 << 20):
    return pl.pallas_call(
        kernel,
        out_shape=[jax.ShapeDtypeStruct(shape, dtype) for shape, dtype in outs],
        in_specs=specs or [VMEM] * len(args),
        out_specs=out_specs or [VMEM] * len(outs),
        scratch_shapes=scratch,
        compiler_params=pltpu.CompilerParams(vmem_limit_bytes=limit),
        cost_estimate=pl.CostEstimate(flops=flops, bytes_accessed=1 << 20, transcendentals=0),
    )(*args)


def make_body(n_tm, n_space):
    lanes = n_tm // 2

    def move(block, turn, swap, shift):
        route = []
        for t in range(n_tm):
            for s in range(n_space):
                y, core = t // 2, t % 2
                t_from = ((y + turn) % lanes) * 2 + (core ^ swap)
                s_from = (s + shift) % n_space
                route.append((t_from * n_space + s_from, t * n_space + s))
        return lax.ppermute(block, ("tm", "space"), route)

    def steps(
        state, obs_start, foot_weight, obs_slot, obs_frac, live_count, obs_values, jacobian, inv_var
    ):
        own = state[0]
        cols, levels = own.shape
        half = cols // 2
        width = 2 * cols
        chan = jacobian.shape[1]
        obs = obs_start.shape[0]

        def flat(vector):
            return vector.reshape(1, -1)

        full, head, tail = call(
            project_kernel,
            [((chan, cols), BF16), ((chan, half), BF16), ((chan, half), BF16)],
            own.T,
            jacobian,
            specs=[HBM, HBM],
            flops=1 << 20,
            scratch=[
                pltpu.VMEM((levels, cols), BF16),
                pltpu.VMEM((levels, chan), BF16),
                pltpu.SemaphoreType.DMA((2,)),
            ],
        )
        (info,) = call(
            functools.partial(info_kernel, cols, n_space),
            [((16, obs), F32)],
            flat(obs_start),
            foot_weight.T,
            flat(obs_slot),
            flat(obs_frac),
        )
        left, right = move(tail, 0, 0, -1), move(head, 0, 0, 1)
        infos = [info] + [move(info, j, 0, 0) for j in range(1, lanes)]
        (wide,) = call(widen_kernel, [((chan, width), BF16)], full, left, right)
        other = move(wide, 0, 1, 0)
        mats = [None] * lanes
        (mats[2],) = call(footprint, [((width, obs), BF16)], infos[2])

        def gather(which):
            outs = call(
                functools.partial(build_gather_kernel, len(which)),
                [((width, obs), BF16)] * len(which) + [((chan, obs), BF16)] * len(which),
                wide,
                other,
                *[infos[j] for j in which],
            )
            for index, j in enumerate(which):
                mats[j] = outs[index]
            return outs[len(which) :]

        (far,) = call(gather_kernel, [((chan, obs), BF16)], wide, other, infos[2], mats[2])
        far = move(far, -2, 0, 0)
        after, before = gather([1, 3])
        after, before = move(after, -1, 0, 0), move(before, 1, 0, 0)
        (kept,) = gather([0])
        values, scale = call(
            values_kernel,
            [((chan, obs), F32), ((chan, chan), F32)],
            obs_values,
            flat(inv_var),
            specs=[HBM, VMEM],
            scratch=[pltpu.VMEM((obs, chan), F32), pltpu.SemaphoreType.DMA],
        )
        gaps, scaled = call(
            functools.partial(depart_kernel, lanes),
            [((chan, obs), F32), ((chan, obs), BF16)],
            live_count,
            kept,
            far,
            after,
            before,
            values,
            scale,
            specs=[SMEM] + [VMEM] * (lanes + 2),
        )
        all_scaled = [scaled] + [move(scaled, j, 0, 0) for j in range(1, lanes)]
        (acc,) = call(spread_first_kernel, [((2 * chan, width), F32)], info, scaled, mats[0])
        (departures,) = call(turn_kernel, [((obs, chan), F32)], gaps)
        for j in range(1, lanes - 1):
            (acc,) = call(
                spread_next_kernel,
                [((2 * chan, width), F32)],
                acc,
                infos[j],
                all_scaled[j],
                mats[j],
            )
        mine, give = call(
            spread_last_kernel,
            [((chan, width), F32), ((chan, width), BF16)],
            acc,
            infos[lanes - 1],
            all_scaled[lanes - 1],
            mats[lanes - 1],
        )
        mid, to_left, to_right = call(
            join_kernel,
            [((chan, cols), F32)] + [((chan, half), BF16)] * 2,
            mine,
            move(give, 0, 1, 0),
        )
        (adjoint,) = call(
            finish_kernel,
            [((levels, 1, cols), F32)],
            mid,
            move(to_right, 0, 0, -1),
            move(to_left, 0, 0, 1),
            jacobian,
            out_specs=[HBM],
            scratch=[pltpu.VMEM((levels, 1, cols), F32), pltpu.SemaphoreType.DMA((2,))],
        )
        return (departures, jnp.transpose(adjoint, (1, 2, 0)))

    return steps


def solution(mesh):
    return jax.shard_map(
        make_body(mesh.shape["tm"], mesh.shape["space"]),
        mesh=mesh,
        in_specs=(
            P("tm", "space", None),
            P(("tm", "space")),
            P(("tm", "space"), None),
            P(("tm", "space")),
            P(("tm", "space")),
            P("tm", "space"),
            P(("tm", "space"), None),
            P(),
            P(),
        ),
        out_specs=(P(("tm", "space"), None), P("tm", "space", None)),
        check_vma=False,
    )
```

```python
import functools

import jax
import jax.numpy as jnp
from jax import lax
from jax.experimental import pallas as pl
from jax.experimental.pallas import tpu as pltpu
from jax.sharding import PartitionSpec as P


F32 = jnp.float32
BF16 = jnp.bfloat16
GROUP = 16


VMEM = pl.BlockSpec(memory_space=pltpu.VMEM)
SMEM = pl.BlockSpec(memory_space=pltpu.SMEM)
HBM = pl.BlockSpec(memory_space=pltpu.HBM)


def held_slots():
    turn = lax.axis_index("tm")
    return turn.astype(F32), (turn ^ 1).astype(F32)


def even_tile():
    return lax.axis_index("space") % 2 == 0


def put_rims(near, far, left, right):
    @pl.when(even_tile())
    def _():
        near[...] = right
        far[...] = left

    @pl.when(jnp.logical_not(even_tile()))
    def _():
        near[...] = left
        far[...] = right


def project_kernel(state, jac, full, near, far, field, levels, sems):
    half = full.shape[1] // 2
    copies = [
        pltpu.make_async_copy(state, field, sems.at[0]),
        pltpu.make_async_copy(jac, levels, sems.at[1]),
    ]
    for copy in copies:
        copy.start()
    for copy in copies:
        copy.wait()
    out = lax.dot_general(
        levels[...], field[...], (((0,), (0,)), ((), ())), preferred_element_type=F32
    ).astype(BF16)
    full[...] = out
    put_rims(near, far, out[:, :half], out[:, half:])


def info_kernel(cols, tiles, start, weight, slot, frac, info):
    base = lax.axis_index("space") * cols - cols // 2
    total = cols * tiles
    local = start[...] - base
    local = jnp.where(local < 0, local + total, local)
    local = jnp.where(local >= total, local - total, local)
    rows = lax.broadcasted_iota(jnp.int32, (8, local.shape[1]), 0)
    extra = jnp.where(rows == 0, local.astype(F32), 0.0)
    extra = jnp.where(rows == 1, slot[...].astype(F32), extra)
    extra = jnp.where(rows == 2, frac[...], extra)
    info[0:8, :] = weight[...].astype(F32)
    info[8:16, :] = extra


def widen_kernel(full, near, far, wide):
    cols = full.shape[1]
    half = cols // 2
    wide[:, half : half + cols] = full[...]

    @pl.when(even_tile())
    def _():
        wide[:, :half] = far[...]
        wide[:, half + cols :] = near[...]

    @pl.when(jnp.logical_not(even_tile()))
    def _():
        wide[:, :half] = near[...]
        wide[:, half + cols :] = far[...]


def footprint(info, mat):
    width, obs = mat.shape
    local = info[8:9, :].astype(jnp.int32)
    low = local & (GROUP - 1)
    high = lax.shift_right_logical(local, 4)
    rows = lax.broadcasted_iota(jnp.int32, (GROUP, obs), 0)
    offset = (rows - low) & (GROUP - 1)
    piece = jnp.zeros((GROUP, obs), F32)
    for k in range(8):
        piece = piece + jnp.where(offset == k, info[k : k + 1, :], 0.0)
    piece = piece.astype(BF16)
    group = (high + jnp.where(rows < low, 1, 0)).astype(F32).astype(BF16)
    zero = jnp.zeros((GROUP, obs), BF16)
    for g in range(width // GROUP):
        mat[g * GROUP : (g + 1) * GROUP, :] = jnp.where(
            group == jnp.full((GROUP, obs), g, BF16), piece, zero
        )


def slot_weight(info, held):
    slot = info[9:10, :]
    frac = info[10:11, :]
    return jnp.where(slot == held, 1.0 - frac, 0.0) + jnp.where(slot + 1.0 == held, frac, 0.0)


def gather_one(field, info, mat, out):
    chan = out.shape[0]
    own_slot, other_slot = held_slots()
    both = jnp.dot(field, mat[...], preferred_element_type=F32)
    first = slot_weight(info, own_slot)
    second = slot_weight(info, other_slot)
    out[...] = (first * both[:chan] + second * both[chan:]).astype(BF16)


def gather_kernel(mine, other, info, mat, out):
    gather_one(jnp.concatenate([mine[...], other[...]], axis=0), info, mat, out)


def build_gather_kernel(n, mine, other, *refs):
    infos, mats, outs = refs[:n], refs[n : 2 * n], refs[2 * n :]
    field = jnp.concatenate([mine[...], other[...]], axis=0)
    for info, mat, out in zip(infos, mats, outs):
        footprint(info, mat)
        gather_one(field, info, mat, out)


def turn_kernel(source, out):
    out[...] = jnp.transpose(source[...])


def values_kernel(source, inv_var, values, scale, held, sem):
    copy = pltpu.make_async_copy(source, held, sem)
    copy.start()
    scale[...] = jnp.transpose(jnp.broadcast_to(inv_var[...], scale.shape))
    copy.wait()
    values[...] = jnp.transpose(held[...])


def depart_kernel(n, count, *refs):
    parts = refs[:n]
    values, scale, gaps, scaled = refs[n:]
    chan, obs = values.shape
    total = parts[0][...].astype(F32)
    for part in parts[1:]:
        total = total + part[...].astype(F32)
    live = lax.broadcasted_iota(jnp.int32, (chan, obs), 1) < count[0, 0]
    gap = jnp.where(live, values[...] - total, 0.0)
    gaps[...] = gap
    scaled[...] = (gap * scale[:, 0:1]).astype(BF16)


def spread_one(info, source, mat):
    own_slot, other_slot = held_slots()
    rows = source[...].astype(F32)
    mine = (slot_weight(info, own_slot) * rows).astype(BF16)
    other = (slot_weight(info, other_slot) * rows).astype(BF16)
    return lax.dot_general(
        jnp.concatenate([mine, other], axis=0),
        mat[...],
        (((1,), (1,)), ((), ())),
        preferred_element_type=F32,
    )


def spread_first_kernel(info, scaled, mat, acc):
    acc[...] = spread_one(info, scaled, mat)


def spread_next_kernel(before, info, scaled, mat, acc):
    acc[...] = before[...] + spread_one(info, scaled, mat)


def spread_last_kernel(before, info, scaled, mat, own, give):
    chan = own.shape[0]
    total = before[...] + spread_one(info, scaled, mat)
    own[...] = total[:chan]
    give[...] = total[chan:].astype(BF16)


def join_kernel(own, got, mid, near, far):
    cols = mid.shape[1]
    half = cols // 2
    mid[...] = own[:, half : half + cols] + got[:, half : half + cols].astype(F32)
    left = (own[:, :half] + got[:, :half].astype(F32)).astype(BF16)
    right = (own[:, half + cols :] + got[:, half + cols :].astype(F32)).astype(BF16)
    put_rims(near, far, left, right)


def finish_kernel(mid, near, far, jac, out, rows, sems):
    half = near.shape[1]
    levels = jac.shape[0]
    cut = (levels // 2 + 15) // 16 * 16
    even = even_tile()
    first = mid[:, :half] + jnp.where(even, far[...], near[...]).astype(F32)
    last = mid[:, half:] + jnp.where(even, near[...], far[...]).astype(F32)
    total = jnp.concatenate([first, last], axis=1).astype(BF16)
    copies = []
    for index, part in enumerate((slice(0, cut), slice(cut, levels))):
        rows[part, 0, :] = jnp.dot(jac[part, :], total, preferred_element_type=F32)
        copy = pltpu.make_async_copy(rows.at[part], out.at[part], sems.at[index])
        copy.start()
        copies.append(copy)
    for copy in copies:
        copy.wait()


def call(kernel, outs, *args, specs=None, out_specs=None, scratch=(), limit=8 << 20, flops=1 << 20):
    return pl.pallas_call(
        kernel,
        out_shape=[jax.ShapeDtypeStruct(shape, dtype) for shape, dtype in outs],
        in_specs=specs or [VMEM] * len(args),
        out_specs=out_specs or [VMEM] * len(outs),
        scratch_shapes=scratch,
        compiler_params=pltpu.CompilerParams(vmem_limit_bytes=limit),
        cost_estimate=pl.CostEstimate(flops=flops, bytes_accessed=1 << 20, transcendentals=0),
    )(*args)


def make_body(n_tm, n_space):
    lanes = n_tm // 2

    def swap(block, y=0, core=0, tile=None):
        partner = {
            None: lambda s: s,
            "near": lambda s: s ^ 1,
            "far": lambda s: (s + 1 if s % 2 else s - 1) % n_space,
        }[tile]
        route = []
        for t in range(n_tm):
            for s in range(n_space):
                other = (t // 2 ^ y) * 2 + (t % 2 ^ core)
                route.append((other * n_space + partner(s), t * n_space + s))
        return lax.ppermute(block, ("tm", "space"), route)

    def steps(
        state, obs_start, foot_weight, obs_slot, obs_frac, live_count, obs_values, jacobian, inv_var
    ):
        own = state[0]
        cols, levels = own.shape
        half = cols // 2
        width = 2 * cols
        chan = jacobian.shape[1]
        obs = obs_start.shape[0]

        def flat(vector):
            return vector.reshape(1, -1)

        full, near, far = call(
            project_kernel,
            [((chan, cols), BF16), ((chan, half), BF16), ((chan, half), BF16)],
            own.T,
            jacobian,
            specs=[HBM, HBM],
            flops=1 << 20,
            scratch=[
                pltpu.VMEM((levels, cols), BF16),
                pltpu.VMEM((levels, chan), BF16),
                pltpu.SemaphoreType.DMA((2,)),
            ],
        )
        (info,) = call(
            functools.partial(info_kernel, cols, n_space),
            [((16, obs), F32)],
            flat(obs_start),
            foot_weight.T,
            flat(obs_slot),
            flat(obs_frac),
        )
        near, far = swap(near, tile="near"), swap(far, tile="far")
        infos = [info] + [swap(info, y=j) for j in range(1, lanes)]
        (wide,) = call(widen_kernel, [((chan, width), BF16)], full, near, far)
        other = swap(wide, core=1)
        mats = [None] * lanes
        (mats[2],) = call(footprint, [((width, obs), BF16)], infos[2])

        def gather(which):
            outs = call(
                functools.partial(build_gather_kernel, len(which)),
                [((width, obs), BF16)] * len(which) + [((chan, obs), BF16)] * len(which),
                wide,
                other,
                *[infos[j] for j in which],
            )
            for index, j in enumerate(which):
                mats[j] = outs[index]
            return outs[len(which) :]

        (far,) = call(gather_kernel, [((chan, obs), BF16)], wide, other, infos[2], mats[2])
        parts = [None] * lanes
        parts[2] = swap(far, y=2)
        for j, part in zip((1, 3), gather([1, 3])):
            parts[j] = swap(part, y=j)
        (parts[0],) = gather([0])
        values, scale = call(
            values_kernel,
            [((chan, obs), F32), ((chan, chan), F32)],
            obs_values,
            flat(inv_var),
            specs=[HBM, VMEM],
            scratch=[pltpu.VMEM((obs, chan), F32), pltpu.SemaphoreType.DMA],
        )
        gaps, scaled = call(
            functools.partial(depart_kernel, lanes),
            [((chan, obs), F32), ((chan, obs), BF16)],
            live_count,
            *parts,
            values,
            scale,
            specs=[SMEM] + [VMEM] * (lanes + 2),
        )
        all_scaled = [scaled] + [swap(scaled, y=j) for j in range(1, lanes)]
        (acc,) = call(spread_first_kernel, [((2 * chan, width), F32)], info, scaled, mats[0])
        (departures,) = call(turn_kernel, [((obs, chan), F32)], gaps)
        for j in range(1, lanes - 1):
            (acc,) = call(
                spread_next_kernel,
                [((2 * chan, width), F32)],
                acc,
                infos[j],
                all_scaled[j],
                mats[j],
            )
        mine, give = call(
            spread_last_kernel,
            [((chan, width), F32), ((chan, width), BF16)],
            acc,
            infos[lanes - 1],
            all_scaled[lanes - 1],
            mats[lanes - 1],
        )
        mid, near, far = call(
            join_kernel,
            [((chan, cols), F32)] + [((chan, half), BF16)] * 2,
            mine,
            swap(give, core=1),
        )
        (adjoint,) = call(
            finish_kernel,
            [((levels, 1, cols), F32)],
            mid,
            swap(near, tile="near"),
            swap(far, tile="far"),
            jacobian,
            out_specs=[HBM],
            scratch=[pltpu.VMEM((levels, 1, cols), F32), pltpu.SemaphoreType.DMA((2,))],
        )
        return (departures, jnp.transpose(adjoint, (1, 2, 0)))

    return steps


def solution(mesh):
    return jax.shard_map(
        make_body(mesh.shape["tm"], mesh.shape["space"]),
        mesh=mesh,
        in_specs=(
            P("tm", "space", None),
            P(("tm", "space")),
            P(("tm", "space"), None),
            P(("tm", "space")),
            P(("tm", "space")),
            P("tm", "space"),
            P(("tm", "space"), None),
            P(),
            P(),
        ),
        out_specs=(P(("tm", "space"), None), P("tm", "space", None)),
        check_vma=False,
    )
```

```python
import functools

import jax
import jax.numpy as jnp
from jax import lax
from jax.experimental import pallas as pl
from jax.experimental.pallas import tpu as pltpu
from jax.sharding import PartitionSpec as P


F32 = jnp.float32
BF16 = jnp.bfloat16
GROUP = 16
FIRST_FLOPS = 1 << 34


VMEM = pl.BlockSpec(memory_space=pltpu.VMEM)
SMEM = pl.BlockSpec(memory_space=pltpu.SMEM)
HBM = pl.BlockSpec(memory_space=pltpu.HBM)


def held_slots():
    turn = lax.axis_index("tm")
    return turn.astype(F32), (turn ^ 1).astype(F32)


def even_tile():
    return lax.axis_index("space") % 2 == 0


def put_rims(near, far, left, right):
    @pl.when(even_tile())
    def _():
        near[...] = right
        far[...] = left

    @pl.when(jnp.logical_not(even_tile()))
    def _():
        near[...] = left
        far[...] = right


def first_kernel(out):
    out[...] = jnp.zeros_like(out)


def project_kernel(first, state, jac, full, near, far):
    half = full.shape[1] // 2
    out = lax.dot_general(
        jac[...], state[...], (((0,), (0,)), ((), ())), preferred_element_type=F32
    ).astype(BF16)
    full[...] = out
    put_rims(near, far, out[:, :half], out[:, half:])


def info_kernel(cols, tiles, first, start, weight, slot, frac, info):
    base = lax.axis_index("space") * cols - cols // 2
    total = cols * tiles
    local = start[...] - base
    local = jnp.where(local < 0, local + total, local)
    local = jnp.where(local >= total, local - total, local)
    rows = lax.broadcasted_iota(jnp.int32, (8, local.shape[1]), 0)
    extra = jnp.where(rows == 0, local.astype(F32), 0.0)
    extra = jnp.where(rows == 1, slot[...].astype(F32), extra)
    extra = jnp.where(rows == 2, frac[...], extra)
    info[0:8, :] = weight[...].astype(F32)
    info[8:16, :] = extra


def widen_kernel(full, near, far, wide):
    cols = full.shape[1]
    half = cols // 2
    wide[:, half : half + cols] = full[...]

    @pl.when(even_tile())
    def _():
        wide[:, :half] = far[...]
        wide[:, half + cols :] = near[...]

    @pl.when(jnp.logical_not(even_tile()))
    def _():
        wide[:, :half] = near[...]
        wide[:, half + cols :] = far[...]


def footprint(info, mat):
    width, obs = mat.shape
    local = info[8:9, :].astype(jnp.int32)
    low = local & (GROUP - 1)
    high = lax.shift_right_logical(local, 4)
    rows = lax.broadcasted_iota(jnp.int32, (GROUP, obs), 0)
    offset = (rows - low) & (GROUP - 1)
    piece = jnp.zeros((GROUP, obs), F32)
    for k in range(8):
        piece = piece + jnp.where(offset == k, info[k : k + 1, :], 0.0)
    piece = piece.astype(BF16)
    group = (high + jnp.where(rows < low, 1, 0)).astype(F32).astype(BF16)
    zero = jnp.zeros((GROUP, obs), BF16)
    for g in range(width // GROUP):
        mat[g * GROUP : (g + 1) * GROUP, :] = jnp.where(
            group == jnp.full((GROUP, obs), g, BF16), piece, zero
        )


def slot_weight(info, held):
    slot = info[9:10, :]
    frac = info[10:11, :]
    return jnp.where(slot == held, 1.0 - frac, 0.0) + jnp.where(slot + 1.0 == held, frac, 0.0)


def gather_one(field, info, mat, out):
    chan = out.shape[0]
    own_slot, other_slot = held_slots()
    both = jnp.dot(field, mat[...], preferred_element_type=F32)
    first = slot_weight(info, own_slot)
    second = slot_weight(info, other_slot)
    out[...] = (first * both[:chan] + second * both[chan:]).astype(BF16)


def gather_kernel(mine, other, info, mat, out):
    gather_one(jnp.concatenate([mine[...], other[...]], axis=0), info, mat, out)


def build_gather_kernel(n, mine, other, *refs):
    infos, mats, outs = refs[:n], refs[n : 2 * n], refs[2 * n :]
    field = jnp.concatenate([mine[...], other[...]], axis=0)
    for info, mat, out in zip(infos, mats, outs):
        footprint(info, mat)
        gather_one(field, info, mat, out)


def turn_kernel(source, out):
    out[...] = jnp.transpose(source[...])


def values_kernel(source, inv_var, values, scale, held, sem):
    copy = pltpu.make_async_copy(source, held, sem)
    copy.start()
    scale[...] = jnp.transpose(jnp.broadcast_to(inv_var[...], scale.shape))
    copy.wait()
    values[...] = jnp.transpose(held[...])


def depart_kernel(n, count, *refs):
    parts = refs[:n]
    values, scale, gaps, scaled = refs[n:]
    chan, obs = values.shape
    total = parts[0][...].astype(F32)
    for part in parts[1:]:
        total = total + part[...].astype(F32)
    live = lax.broadcasted_iota(jnp.int32, (chan, obs), 1) < count[0, 0]
    gap = jnp.where(live, values[...] - total, 0.0)
    gaps[...] = gap
    scaled[...] = (gap * scale[:, 0:1]).astype(BF16)


def spread_one(info, source, mat):
    own_slot, other_slot = held_slots()
    rows = source[...].astype(F32)
    mine = (slot_weight(info, own_slot) * rows).astype(BF16)
    other = (slot_weight(info, other_slot) * rows).astype(BF16)
    return lax.dot_general(
        jnp.concatenate([mine, other], axis=0),
        mat[...],
        (((1,), (1,)), ((), ())),
        preferred_element_type=F32,
    )


def spread_first_kernel(info, scaled, mat, acc):
    acc[...] = spread_one(info, scaled, mat)


def spread_next_kernel(before, info, scaled, mat, acc):
    acc[...] = before[...] + spread_one(info, scaled, mat)


def spread_last_kernel(before, info, scaled, mat, own, give):
    chan = own.shape[0]
    total = before[...] + spread_one(info, scaled, mat)
    own[...] = total[:chan]
    give[...] = total[chan:].astype(BF16)


def join_kernel(own, got, mid, near, far):
    cols = mid.shape[1]
    half = cols // 2
    mid[...] = own[:, half : half + cols] + got[:, half : half + cols].astype(F32)
    left = (own[:, :half] + got[:, :half].astype(F32)).astype(BF16)
    right = (own[:, half + cols :] + got[:, half + cols :].astype(F32)).astype(BF16)
    put_rims(near, far, left, right)


def finish_kernel(mid, near, far, jac, out, rows, sems):
    half = near.shape[1]
    levels = jac.shape[0]
    cut = (levels // 2 + 15) // 16 * 16
    even = even_tile()
    first = mid[:, :half] + jnp.where(even, far[...], near[...]).astype(F32)
    last = mid[:, half:] + jnp.where(even, near[...], far[...]).astype(F32)
    total = jnp.concatenate([first, last], axis=1).astype(BF16)
    copies = []
    for index, part in enumerate((slice(0, cut), slice(cut, levels))):
        rows[part, 0, :] = jnp.dot(jac[part, :], total, preferred_element_type=F32)
        copy = pltpu.make_async_copy(rows.at[part], out.at[part], sems.at[index])
        copy.start()
        copies.append(copy)
    for copy in copies:
        copy.wait()


def call(kernel, outs, *args, specs=None, out_specs=None, scratch=(), limit=8 << 20, flops=1 << 20):
    return pl.pallas_call(
        kernel,
        out_shape=[jax.ShapeDtypeStruct(shape, dtype) for shape, dtype in outs],
        in_specs=specs or [VMEM] * len(args),
        out_specs=out_specs or [VMEM] * len(outs),
        scratch_shapes=scratch,
        compiler_params=pltpu.CompilerParams(vmem_limit_bytes=limit),
        cost_estimate=pl.CostEstimate(flops=flops, bytes_accessed=1 << 20, transcendentals=0),
    )(*args)


def make_body(n_tm, n_space):
    lanes = n_tm // 2

    def swap(block, y=0, core=0, tile=None):
        partner = {
            None: lambda s: s,
            "near": lambda s: s ^ 1,
            "far": lambda s: (s + 1 if s % 2 else s - 1) % n_space,
        }[tile]
        route = []
        for t in range(n_tm):
            for s in range(n_space):
                other = (t // 2 ^ y) * 2 + (t % 2 ^ core)
                route.append((other * n_space + partner(s), t * n_space + s))
        return lax.ppermute(block, ("tm", "space"), route)

    def steps(
        state, obs_start, foot_weight, obs_slot, obs_frac, live_count, obs_values, jacobian, inv_var
    ):
        own = state[0]
        cols, levels = own.shape
        half = cols // 2
        width = 2 * cols
        chan = jacobian.shape[1]
        obs = obs_start.shape[0]

        def flat(vector):
            return vector.reshape(1, -1)

        (first,) = call(first_kernel, [((8, 128), F32)], flops=FIRST_FLOPS)
        (info,) = call(
            functools.partial(info_kernel, cols, n_space),
            [((16, obs), F32)],
            first,
            flat(obs_start),
            foot_weight.T,
            flat(obs_slot),
            flat(obs_frac),
            flops=FIRST_FLOPS,
        )
        full, near, far = call(
            project_kernel,
            [((chan, cols), BF16), ((chan, half), BF16), ((chan, half), BF16)],
            info,
            own.T,
            jacobian,
        )
        near, far = swap(near, tile="near"), swap(far, tile="far")
        infos = [info] + [swap(info, y=j) for j in range(1, lanes)]
        (wide,) = call(widen_kernel, [((chan, width), BF16)], full, near, far)
        other = swap(wide, core=1)
        mats = [None] * lanes
        (mats[2],) = call(footprint, [((width, obs), BF16)], infos[2])

        def gather(which):
            outs = call(
                functools.partial(build_gather_kernel, len(which)),
                [((width, obs), BF16)] * len(which) + [((chan, obs), BF16)] * len(which),
                wide,
                other,
                *[infos[j] for j in which],
            )
            for index, j in enumerate(which):
                mats[j] = outs[index]
            return outs[len(which) :]

        (far,) = call(gather_kernel, [((chan, obs), BF16)], wide, other, infos[2], mats[2])
        parts = [None] * lanes
        parts[2] = swap(far, y=2)
        for j, part in zip((1, 3), gather([1, 3])):
            parts[j] = swap(part, y=j)
        (parts[0],) = gather([0])
        values, scale = call(
            values_kernel,
            [((chan, obs), F32), ((chan, chan), F32)],
            obs_values,
            flat(inv_var),
            specs=[HBM, VMEM],
            scratch=[pltpu.VMEM((obs, chan), F32), pltpu.SemaphoreType.DMA],
        )
        gaps, scaled = call(
            functools.partial(depart_kernel, lanes),
            [((chan, obs), F32), ((chan, obs), BF16)],
            live_count,
            *parts,
            values,
            scale,
            specs=[SMEM] + [VMEM] * (lanes + 2),
        )
        all_scaled = [scaled] + [swap(scaled, y=j) for j in range(1, lanes)]
        (acc,) = call(spread_first_kernel, [((2 * chan, width), F32)], info, scaled, mats[0])
        (departures,) = call(turn_kernel, [((obs, chan), F32)], gaps)
        for j in range(1, lanes - 1):
            (acc,) = call(
                spread_next_kernel,
                [((2 * chan, width), F32)],
                acc,
                infos[j],
                all_scaled[j],
                mats[j],
            )
        mine, give = call(
            spread_last_kernel,
            [((chan, width), F32), ((chan, width), BF16)],
            acc,
            infos[lanes - 1],
            all_scaled[lanes - 1],
            mats[lanes - 1],
        )
        mid, near, far = call(
            join_kernel,
            [((chan, cols), F32)] + [((chan, half), BF16)] * 2,
            mine,
            swap(give, core=1),
        )
        (adjoint,) = call(
            finish_kernel,
            [((levels, 1, cols), F32)],
            mid,
            swap(near, tile="near"),
            swap(far, tile="far"),
            jacobian,
            out_specs=[HBM],
            scratch=[pltpu.VMEM((levels, 1, cols), F32), pltpu.SemaphoreType.DMA((2,))],
        )
        return (departures, jnp.transpose(adjoint, (1, 2, 0)))

    return steps


def solution(mesh):
    return jax.shard_map(
        make_body(mesh.shape["tm"], mesh.shape["space"]),
        mesh=mesh,
        in_specs=(
            P("tm", "space", None),
            P(("tm", "space")),
            P(("tm", "space"), None),
            P(("tm", "space")),
            P(("tm", "space")),
            P("tm", "space"),
            P(("tm", "space"), None),
            P(),
            P(),
        ),
        out_specs=(P(("tm", "space"), None), P("tm", "space", None)),
        check_vma=False,
    )
```

```python
import functools

import jax
import jax.numpy as jnp
from jax import lax
from jax.experimental import pallas as pl
from jax.experimental.pallas import tpu as pltpu
from jax.sharding import PartitionSpec as P


F32 = jnp.float32
BF16 = jnp.bfloat16
GROUP = 16
SWAP_ORDER = (2, 3, 1)
FIRST_FLOPS = 1 << 34


VMEM = pl.BlockSpec(memory_space=pltpu.VMEM)
SMEM = pl.BlockSpec(memory_space=pltpu.SMEM)
HBM = pl.BlockSpec(memory_space=pltpu.HBM)


def held_slots():
    turn = lax.axis_index("tm")
    return turn.astype(F32), (turn ^ 1).astype(F32)


def even_tile():
    return lax.axis_index("space") % 2 == 0


def put_rims(near, far, left, right):
    @pl.when(even_tile())
    def _():
        near[...] = right
        far[...] = left

    @pl.when(jnp.logical_not(even_tile()))
    def _():
        near[...] = left
        far[...] = right


def first_kernel(out):
    out[...] = jnp.zeros_like(out)


def project_kernel(first, state, jac, full, near, far):
    half = full.shape[1] // 2
    out = lax.dot_general(
        jac[...], state[...], (((0,), (0,)), ((), ())), preferred_element_type=F32
    ).astype(BF16)
    full[...] = out
    put_rims(near, far, out[:, :half], out[:, half:])


def info_kernel(cols, tiles, start, weight, slot, frac, info):
    base = lax.axis_index("space") * cols - cols // 2
    total = cols * tiles
    local = start[...] - base
    local = jnp.where(local < 0, local + total, local)
    local = jnp.where(local >= total, local - total, local)
    rows = lax.broadcasted_iota(jnp.int32, (8, local.shape[1]), 0)
    extra = jnp.where(rows == 0, local.astype(F32), 0.0)
    extra = jnp.where(rows == 1, slot[...].astype(F32), extra)
    extra = jnp.where(rows == 2, frac[...], extra)
    info[0:8, :] = weight[...].astype(F32)
    info[8:16, :] = extra


def widen_kernel(full, near, far, wide):
    cols = full.shape[1]
    half = cols // 2
    wide[:, half : half + cols] = full[...]

    @pl.when(even_tile())
    def _():
        wide[:, :half] = far[...]
        wide[:, half + cols :] = near[...]

    @pl.when(jnp.logical_not(even_tile()))
    def _():
        wide[:, :half] = near[...]
        wide[:, half + cols :] = far[...]


def footprint(info, mat):
    width, obs = mat.shape
    local = info[8:9, :].astype(jnp.int32)
    low = local & (GROUP - 1)
    high = lax.shift_right_logical(local, 4)
    rows = lax.broadcasted_iota(jnp.int32, (GROUP, obs), 0)
    offset = (rows - low) & (GROUP - 1)
    piece = jnp.zeros((GROUP, obs), F32)
    for k in range(8):
        piece = piece + jnp.where(offset == k, info[k : k + 1, :], 0.0)
    piece = piece.astype(BF16)
    group = (high + jnp.where(rows < low, 1, 0)).astype(F32).astype(BF16)
    zero = jnp.zeros((GROUP, obs), BF16)
    for g in range(width // GROUP):
        mat[g * GROUP : (g + 1) * GROUP, :] = jnp.where(
            group == jnp.full((GROUP, obs), g, BF16), piece, zero
        )


def slot_weight(info, held):
    slot = info[9:10, :]
    frac = info[10:11, :]
    return jnp.where(slot == held, 1.0 - frac, 0.0) + jnp.where(slot + 1.0 == held, frac, 0.0)


def gather_one(field, info, mat, out):
    chan = out.shape[0]
    own_slot, other_slot = held_slots()
    both = jnp.dot(field, mat[...], preferred_element_type=F32)
    first = slot_weight(info, own_slot)
    second = slot_weight(info, other_slot)
    out[...] = (first * both[:chan] + second * both[chan:]).astype(BF16)


def gather_kernel(mine, other, info, mat, out):
    gather_one(jnp.concatenate([mine[...], other[...]], axis=0), info, mat, out)


def build_gather_kernel(n, mine, other, *refs):
    infos, mats, outs = refs[:n], refs[n : 2 * n], refs[2 * n :]
    field = jnp.concatenate([mine[...], other[...]], axis=0)
    for info, mat, out in zip(infos, mats, outs):
        footprint(info, mat)
        gather_one(field, info, mat, out)


def turn_kernel(source, out):
    out[...] = jnp.transpose(source[...])


def values_kernel(source, inv_var, values, scale, held, sem):
    copy = pltpu.make_async_copy(source, held, sem)
    copy.start()
    scale[...] = jnp.transpose(jnp.broadcast_to(inv_var[...], scale.shape))
    copy.wait()
    values[...] = jnp.transpose(held[...])


def depart_kernel(n, count, *refs):
    parts = refs[:n]
    values, scale, gaps, scaled = refs[n:]
    chan, obs = values.shape
    total = parts[0][...].astype(F32)
    for part in parts[1:]:
        total = total + part[...].astype(F32)
    live = lax.broadcasted_iota(jnp.int32, (chan, obs), 1) < count[0, 0]
    gap = jnp.where(live, values[...] - total, 0.0)
    gaps[...] = gap
    scaled[...] = (gap * scale[:, 0:1]).astype(BF16)


def spread_one(info, source, mat):
    own_slot, other_slot = held_slots()
    rows = source[...].astype(F32)
    mine = (slot_weight(info, own_slot) * rows).astype(BF16)
    other = (slot_weight(info, other_slot) * rows).astype(BF16)
    return lax.dot_general(
        jnp.concatenate([mine, other], axis=0),
        mat[...],
        (((1,), (1,)), ((), ())),
        preferred_element_type=F32,
    )


def spread_first_kernel(info, scaled, mat, acc):
    acc[...] = spread_one(info, scaled, mat)


def spread_next_kernel(before, info, scaled, mat, acc):
    acc[...] = before[...] + spread_one(info, scaled, mat)


def spread_last_kernel(before, info, scaled, mat, own, give):
    chan = own.shape[0]
    total = before[...] + spread_one(info, scaled, mat)
    own[...] = total[:chan]
    give[...] = total[chan:].astype(BF16)


def join_kernel(own, got, mid, near, far):
    cols = mid.shape[1]
    half = cols // 2
    mid[...] = own[:, half : half + cols] + got[:, half : half + cols].astype(F32)
    left = (own[:, :half] + got[:, :half].astype(F32)).astype(BF16)
    right = (own[:, half + cols :] + got[:, half + cols :].astype(F32)).astype(BF16)
    put_rims(near, far, left, right)


def finish_kernel(mid, near, far, jac, out, rows, sems):
    half = near.shape[1]
    levels = jac.shape[0]
    cut = (levels // 2 + 15) // 16 * 16
    even = even_tile()
    first = mid[:, :half] + jnp.where(even, far[...], near[...]).astype(F32)
    last = mid[:, half:] + jnp.where(even, near[...], far[...]).astype(F32)
    total = jnp.concatenate([first, last], axis=1).astype(BF16)
    copies = []
    for index, part in enumerate((slice(0, cut), slice(cut, levels))):
        rows[part, 0, :] = jnp.dot(jac[part, :], total, preferred_element_type=F32)
        copy = pltpu.make_async_copy(rows.at[part], out.at[part], sems.at[index])
        copy.start()
        copies.append(copy)
    for copy in copies:
        copy.wait()


def call(kernel, outs, *args, specs=None, out_specs=None, scratch=(), limit=8 << 20, flops=1 << 20):
    return pl.pallas_call(
        kernel,
        out_shape=[jax.ShapeDtypeStruct(shape, dtype) for shape, dtype in outs],
        in_specs=specs or [VMEM] * len(args),
        out_specs=out_specs or [VMEM] * len(outs),
        scratch_shapes=scratch,
        compiler_params=pltpu.CompilerParams(vmem_limit_bytes=limit),
        cost_estimate=pl.CostEstimate(flops=flops, bytes_accessed=1 << 20, transcendentals=0),
    )(*args)


def make_body(n_tm, n_space):
    lanes = n_tm // 2

    def swap(block, y=0, core=0, tile=None):
        partner = {
            None: lambda s: s,
            "near": lambda s: s ^ 1,
            "far": lambda s: (s + 1 if s % 2 else s - 1) % n_space,
        }[tile]
        route = []
        for t in range(n_tm):
            for s in range(n_space):
                other = (t // 2 ^ y) * 2 + (t % 2 ^ core)
                route.append((other * n_space + partner(s), t * n_space + s))
        return lax.ppermute(block, ("tm", "space"), route)

    def steps(
        state, obs_start, foot_weight, obs_slot, obs_frac, live_count, obs_values, jacobian, inv_var
    ):
        own = state[0]
        cols, levels = own.shape
        half = cols // 2
        width = 2 * cols
        chan = jacobian.shape[1]
        obs = obs_start.shape[0]

        def flat(vector):
            return vector.reshape(1, -1)

        (first,) = call(first_kernel, [((8, 128), F32)], flops=FIRST_FLOPS)
        full, near, far = call(
            project_kernel,
            [((chan, cols), BF16), ((chan, half), BF16), ((chan, half), BF16)],
            first,
            own.T,
            jacobian,
        )
        (info,) = call(
            functools.partial(info_kernel, cols, n_space),
            [((16, obs), F32)],
            flat(obs_start),
            foot_weight.T,
            flat(obs_slot),
            flat(obs_frac),
        )
        near, far = swap(near, tile="near"), swap(far, tile="far")
        infos = [info] + [swap(info, y=j) for j in range(1, lanes)]
        (wide,) = call(widen_kernel, [((chan, width), BF16)], full, near, far)
        other = swap(wide, core=1)
        mats = [None] * lanes
        (mats[2],) = call(footprint, [((width, obs), BF16)], infos[2])

        def gather(which):
            outs = call(
                functools.partial(build_gather_kernel, len(which)),
                [((width, obs), BF16)] * len(which) + [((chan, obs), BF16)] * len(which),
                wide,
                other,
                *[infos[j] for j in which],
            )
            for index, j in enumerate(which):
                mats[j] = outs[index]
            return outs[len(which) :]

        (far,) = call(gather_kernel, [((chan, obs), BF16)], wide, other, infos[2], mats[2])
        parts = [None] * lanes
        parts[2] = swap(far, y=2)
        for j, part in zip((3, 1), gather([3, 1])):
            parts[j] = swap(part, y=j)
        (parts[0],) = gather([0])
        values, scale = call(
            values_kernel,
            [((chan, obs), F32), ((chan, chan), F32)],
            obs_values,
            flat(inv_var),
            specs=[HBM, VMEM],
            scratch=[pltpu.VMEM((obs, chan), F32), pltpu.SemaphoreType.DMA],
        )
        gaps, scaled = call(
            functools.partial(depart_kernel, lanes),
            [((chan, obs), F32), ((chan, obs), BF16)],
            live_count,
            *parts,
            values,
            scale,
            specs=[SMEM] + [VMEM] * (lanes + 2),
        )
        all_scaled = [scaled] + [swap(scaled, y=j) for j in range(1, lanes)]
        (acc,) = call(spread_first_kernel, [((2 * chan, width), F32)], info, scaled, mats[0])
        (departures,) = call(turn_kernel, [((obs, chan), F32)], gaps)
        *early, last = SWAP_ORDER
        for j in early:
            (acc,) = call(
                spread_next_kernel,
                [((2 * chan, width), F32)],
                acc,
                infos[j],
                all_scaled[j],
                mats[j],
            )
        mine, give = call(
            spread_last_kernel,
            [((chan, width), F32), ((chan, width), BF16)],
            acc,
            infos[last],
            all_scaled[last],
            mats[last],
        )
        mid, near, far = call(
            join_kernel,
            [((chan, cols), F32)] + [((chan, half), BF16)] * 2,
            mine,
            swap(give, core=1),
        )
        (adjoint,) = call(
            finish_kernel,
            [((levels, 1, cols), F32)],
            mid,
            swap(near, tile="near"),
            swap(far, tile="far"),
            jacobian,
            out_specs=[HBM],
            scratch=[pltpu.VMEM((levels, 1, cols), F32), pltpu.SemaphoreType.DMA((2,))],
        )
        return (departures, jnp.transpose(adjoint, (1, 2, 0)))

    return steps


def solution(mesh):
    return jax.shard_map(
        make_body(mesh.shape["tm"], mesh.shape["space"]),
        mesh=mesh,
        in_specs=(
            P("tm", "space", None),
            P(("tm", "space")),
            P(("tm", "space"), None),
            P(("tm", "space")),
            P(("tm", "space")),
            P("tm", "space"),
            P(("tm", "space"), None),
            P(),
            P(),
        ),
        out_specs=(P(("tm", "space"), None), P("tm", "space", None)),
        check_vma=False,
    )
```

```python
import functools

import jax
import jax.numpy as jnp
from jax import lax
from jax.experimental import pallas as pl
from jax.experimental.pallas import tpu as pltpu
from jax.sharding import PartitionSpec as P


F32 = jnp.float32
BF16 = jnp.bfloat16
GROUP = 16
FIRST_FLOPS = 1 << 34


VMEM = pl.BlockSpec(memory_space=pltpu.VMEM)
SMEM = pl.BlockSpec(memory_space=pltpu.SMEM)
HBM = pl.BlockSpec(memory_space=pltpu.HBM)


def held_slots():
    turn = lax.axis_index("tm")
    return turn.astype(F32), (turn ^ 1).astype(F32)


def even_tile():
    return lax.axis_index("space") % 2 == 0


def put_rims(near, far, left, right):
    @pl.when(even_tile())
    def _():
        near[...] = right
        far[...] = left

    @pl.when(jnp.logical_not(even_tile()))
    def _():
        near[...] = left
        far[...] = right


def first_kernel(out):
    out[...] = jnp.zeros_like(out)


def enter_kernel(tiles, first, state, jac, start, weight, slot, frac, full, near, far, info):
    cols = full.shape[1]
    half = cols // 2
    out = lax.dot_general(
        jac[...], state[...], (((0,), (0,)), ((), ())), preferred_element_type=F32
    ).astype(BF16)
    full[...] = out
    put_rims(near, far, out[:, :half], out[:, half:])
    base = lax.axis_index("space") * cols - half
    total = cols * tiles
    local = start[...] - base
    local = jnp.where(local < 0, local + total, local)
    local = jnp.where(local >= total, local - total, local)
    rows = lax.broadcasted_iota(jnp.int32, (8, local.shape[1]), 0)
    extra = jnp.where(rows == 0, local.astype(F32), 0.0)
    extra = jnp.where(rows == 1, slot[...].astype(F32), extra)
    extra = jnp.where(rows == 2, frac[...], extra)
    info[0:8, :] = weight[...].astype(F32)
    info[8:16, :] = extra


def widen_kernel(full, near, far, wide):
    cols = full.shape[1]
    half = cols // 2
    wide[:, half : half + cols] = full[...]

    @pl.when(even_tile())
    def _():
        wide[:, :half] = far[...]
        wide[:, half + cols :] = near[...]

    @pl.when(jnp.logical_not(even_tile()))
    def _():
        wide[:, :half] = near[...]
        wide[:, half + cols :] = far[...]


def footprint(info, mat):
    width, obs = mat.shape
    local = info[8:9, :].astype(jnp.int32)
    low = local & (GROUP - 1)
    high = lax.shift_right_logical(local, 4)
    rows = lax.broadcasted_iota(jnp.int32, (GROUP, obs), 0)
    offset = (rows - low) & (GROUP - 1)
    piece = jnp.zeros((GROUP, obs), F32)
    for k in range(8):
        piece = piece + jnp.where(offset == k, info[k : k + 1, :], 0.0)
    piece = piece.astype(BF16)
    group = (high + jnp.where(rows < low, 1, 0)).astype(F32).astype(BF16)
    zero = jnp.zeros((GROUP, obs), BF16)
    for g in range(width // GROUP):
        mat[g * GROUP : (g + 1) * GROUP, :] = jnp.where(
            group == jnp.full((GROUP, obs), g, BF16), piece, zero
        )


def slot_weight(info, held):
    slot = info[9:10, :]
    frac = info[10:11, :]
    return jnp.where(slot == held, 1.0 - frac, 0.0) + jnp.where(slot + 1.0 == held, frac, 0.0)


def gather_one(field, info, mat, out):
    chan = out.shape[0]
    own_slot, other_slot = held_slots()
    both = jnp.dot(field, mat[...], preferred_element_type=F32)
    first = slot_weight(info, own_slot)
    second = slot_weight(info, other_slot)
    out[...] = (first * both[:chan] + second * both[chan:]).astype(BF16)


def gather_kernel(mine, other, info, mat, out):
    gather_one(jnp.concatenate([mine[...], other[...]], axis=0), info, mat, out)


def build_gather_kernel(n, mine, other, *refs):
    infos, mats, outs = refs[:n], refs[n : 2 * n], refs[2 * n :]
    field = jnp.concatenate([mine[...], other[...]], axis=0)
    for info, mat, out in zip(infos, mats, outs):
        footprint(info, mat)
        gather_one(field, info, mat, out)


def turn_kernel(source, out):
    out[...] = jnp.transpose(source[...])


def values_kernel(source, inv_var, values, scale, held, sem):
    copy = pltpu.make_async_copy(source, held, sem)
    copy.start()
    scale[...] = jnp.transpose(jnp.broadcast_to(inv_var[...], scale.shape))
    copy.wait()
    values[...] = jnp.transpose(held[...])


def depart_kernel(n, count, *refs):
    parts = refs[:n]
    values, scale, gaps, scaled = refs[n:]
    chan, obs = values.shape
    total = parts[0][...].astype(F32)
    for part in parts[1:]:
        total = total + part[...].astype(F32)
    live = lax.broadcasted_iota(jnp.int32, (chan, obs), 1) < count[0, 0]
    gap = jnp.where(live, values[...] - total, 0.0)
    gaps[...] = gap
    scaled[...] = (gap * scale[:, 0:1]).astype(BF16)


def weighted(info, source, slot):
    return (slot_weight(info, slot) * source[...].astype(F32)).astype(BF16)


def spread_rows(rows, mat):
    return lax.dot_general(
        rows, mat[...], (((1,), (1,)), ((), ())), preferred_element_type=F32
    )


def spread_one(info, source, mat):
    rows = [weighted(info, source, slot) for slot in held_slots()]
    return spread_rows(jnp.concatenate(rows, axis=0), mat)


def spread_first_kernel(info, scaled, mat, acc):
    acc[...] = spread_one(info, scaled, mat)


def spread_next_kernel(before, info, scaled, mat, acc):
    acc[...] = before[...] + spread_one(info, scaled, mat)


def spread_give_kernel(before, info, scaled, mat, give):
    chan = give.shape[0]
    part = spread_rows(weighted(info, scaled, held_slots()[1]), mat)
    give[...] = (before[chan:, :] + part).astype(BF16)


def spread_keep_kernel(before, info, scaled, mat, own):
    chan = own.shape[0]
    own[...] = before[:chan, :] + spread_rows(weighted(info, scaled, held_slots()[0]), mat)


def join_kernel(own, got, mid, near, far):
    cols = mid.shape[1]
    half = cols // 2
    mid[...] = own[:, half : half + cols] + got[:, half : half + cols].astype(F32)
    left = (own[:, :half] + got[:, :half].astype(F32)).astype(BF16)
    right = (own[:, half + cols :] + got[:, half + cols :].astype(F32)).astype(BF16)
    put_rims(near, far, left, right)


def finish_kernel(mid, near, far, jac, out, rows, sems):
    half = near.shape[1]
    levels = jac.shape[0]
    cut = (levels // 2 + 15) // 16 * 16
    even = even_tile()
    first = mid[:, :half] + jnp.where(even, far[...], near[...]).astype(F32)
    last = mid[:, half:] + jnp.where(even, near[...], far[...]).astype(F32)
    total = jnp.concatenate([first, last], axis=1).astype(BF16)
    copies = []
    for index, part in enumerate((slice(0, cut), slice(cut, levels))):
        rows[part, 0, :] = jnp.dot(jac[part, :], total, preferred_element_type=F32)
        copy = pltpu.make_async_copy(rows.at[part], out.at[part], sems.at[index])
        copy.start()
        copies.append(copy)
    for copy in copies:
        copy.wait()


def call(kernel, outs, *args, specs=None, out_specs=None, scratch=(), limit=8 << 20, flops=1 << 20):
    return pl.pallas_call(
        kernel,
        out_shape=[jax.ShapeDtypeStruct(shape, dtype) for shape, dtype in outs],
        in_specs=specs or [VMEM] * len(args),
        out_specs=out_specs or [VMEM] * len(outs),
        scratch_shapes=scratch,
        compiler_params=pltpu.CompilerParams(vmem_limit_bytes=limit),
        cost_estimate=pl.CostEstimate(flops=flops, bytes_accessed=1 << 20, transcendentals=0),
    )(*args)


def make_body(n_tm, n_space):
    lanes = n_tm // 2

    def swap(block, y=0, core=0, tile=None):
        partner = {
            None: lambda s: s,
            "near": lambda s: s ^ 1,
            "far": lambda s: (s + 1 if s % 2 else s - 1) % n_space,
        }[tile]
        route = []
        for t in range(n_tm):
            for s in range(n_space):
                other = (t // 2 ^ y) * 2 + (t % 2 ^ core)
                route.append((other * n_space + partner(s), t * n_space + s))
        return lax.ppermute(block, ("tm", "space"), route)

    def steps(
        state, obs_start, foot_weight, obs_slot, obs_frac, live_count, obs_values, jacobian, inv_var
    ):
        own = state[0]
        cols, levels = own.shape
        half = cols // 2
        width = 2 * cols
        chan = jacobian.shape[1]
        obs = obs_start.shape[0]

        def flat(vector):
            return vector.reshape(1, -1)

        (first,) = call(first_kernel, [((8, 128), F32)], flops=FIRST_FLOPS)
        full, near, far, info = call(
            functools.partial(enter_kernel, n_space),
            [
                ((chan, cols), BF16),
                ((chan, half), BF16),
                ((chan, half), BF16),
                ((16, obs), F32),
            ],
            first,
            own.T,
            jacobian,
            flat(obs_start),
            foot_weight.T,
            flat(obs_slot),
            flat(obs_frac),
        )
        near, far = swap(near, tile="near"), swap(far, tile="far")
        infos = [info] + [swap(info, y=j) for j in range(1, lanes)]
        (wide,) = call(widen_kernel, [((chan, width), BF16)], full, near, far)
        other = swap(wide, core=1)
        mats = [None] * lanes
        (mats[2],) = call(footprint, [((width, obs), BF16)], infos[2])

        def gather(which):
            outs = call(
                functools.partial(build_gather_kernel, len(which)),
                [((width, obs), BF16)] * len(which) + [((chan, obs), BF16)] * len(which),
                wide,
                other,
                *[infos[j] for j in which],
            )
            for index, j in enumerate(which):
                mats[j] = outs[index]
            return outs[len(which) :]

        (far,) = call(gather_kernel, [((chan, obs), BF16)], wide, other, infos[2], mats[2])
        parts = [None] * lanes
        parts[2] = swap(far, y=2)
        for j in (1, 3):
            (part,) = gather([j])
            parts[j] = swap(part, y=j)
        (parts[0],) = gather([0])
        values, scale = call(
            values_kernel,
            [((chan, obs), F32), ((chan, chan), F32)],
            obs_values,
            flat(inv_var),
            specs=[HBM, VMEM],
            scratch=[pltpu.VMEM((obs, chan), F32), pltpu.SemaphoreType.DMA],
        )
        gaps, scaled = call(
            functools.partial(depart_kernel, lanes),
            [((chan, obs), F32), ((chan, obs), BF16)],
            live_count,
            *parts,
            values,
            scale,
            specs=[SMEM] + [VMEM] * (lanes + 2),
        )
        all_scaled = [scaled] + [swap(scaled, y=j) for j in range(1, lanes)]
        (acc,) = call(spread_first_kernel, [((2 * chan, width), F32)], info, scaled, mats[0])
        (departures,) = call(turn_kernel, [((obs, chan), F32)], gaps)
        for j in range(1, lanes - 1):
            (acc,) = call(
                spread_next_kernel,
                [((2 * chan, width), F32)],
                acc,
                infos[j],
                all_scaled[j],
                mats[j],
            )
        rest = (acc, infos[lanes - 1], all_scaled[lanes - 1], mats[lanes - 1])
        (give,) = call(spread_give_kernel, [((chan, width), BF16)], *rest)
        give = swap(give, core=1)
        (mine,) = call(spread_keep_kernel, [((chan, width), F32)], *rest)
        mid, near, far = call(
            join_kernel, [((chan, cols), F32)] + [((chan, half), BF16)] * 2, mine, give
        )
        (adjoint,) = call(
            finish_kernel,
            [((levels, 1, cols), F32)],
            mid,
            swap(near, tile="near"),
            swap(far, tile="far"),
            jacobian,
            out_specs=[HBM],
            scratch=[pltpu.VMEM((levels, 1, cols), F32), pltpu.SemaphoreType.DMA((2,))],
        )
        return (departures, jnp.transpose(adjoint, (1, 2, 0)))

    return steps


def solution(mesh):
    return jax.shard_map(
        make_body(mesh.shape["tm"], mesh.shape["space"]),
        mesh=mesh,
        in_specs=(
            P("tm", "space", None),
            P(("tm", "space")),
            P(("tm", "space"), None),
            P(("tm", "space")),
            P(("tm", "space")),
            P("tm", "space"),
            P(("tm", "space"), None),
            P(),
            P(),
        ),
        out_specs=(P(("tm", "space"), None), P("tm", "space", None)),
        check_vma=False,
    )
```

```python
import functools

import jax
import jax.numpy as jnp
from jax import lax
from jax.experimental import pallas as pl
from jax.experimental.pallas import tpu as pltpu
from jax.sharding import PartitionSpec as P


F32 = jnp.float32
BF16 = jnp.bfloat16
GROUP = 16
SWAP_ORDER = (2, 3, 1)
FIRST_FLOPS = 1 << 34


VMEM = pl.BlockSpec(memory_space=pltpu.VMEM)
SMEM = pl.BlockSpec(memory_space=pltpu.SMEM)
HBM = pl.BlockSpec(memory_space=pltpu.HBM)


def held_slots():
    turn = lax.axis_index("tm")
    return turn.astype(F32), (turn ^ 1).astype(F32)


def even_tile():
    return lax.axis_index("space") % 2 == 0


def put_rims(near, far, left, right):
    @pl.when(even_tile())
    def _():
        near[...] = right
        far[...] = left

    @pl.when(jnp.logical_not(even_tile()))
    def _():
        near[...] = left
        far[...] = right


def first_kernel(out):
    out[...] = jnp.zeros_like(out)


def enter_kernel(tiles, first, state, jac, start, weight, slot, frac, full, near, far, info):
    cols = full.shape[1]
    half = cols // 2
    out = lax.dot_general(
        jac[...], state[...], (((0,), (0,)), ((), ())), preferred_element_type=F32
    ).astype(BF16)
    full[...] = out
    put_rims(near, far, out[:, :half], out[:, half:])
    base = lax.axis_index("space") * cols - half
    total = cols * tiles
    local = start[...] - base
    local = jnp.where(local < 0, local + total, local)
    local = jnp.where(local >= total, local - total, local)
    rows = lax.broadcasted_iota(jnp.int32, (8, local.shape[1]), 0)
    extra = jnp.where(rows == 0, local.astype(F32), 0.0)
    extra = jnp.where(rows == 1, slot[...].astype(F32), extra)
    extra = jnp.where(rows == 2, frac[...], extra)
    info[0:8, :] = weight[...].astype(F32)
    info[8:16, :] = extra


def widen_kernel(full, near, far, wide):
    cols = full.shape[1]
    half = cols // 2
    wide[:, half : half + cols] = full[...]

    @pl.when(even_tile())
    def _():
        wide[:, :half] = far[...]
        wide[:, half + cols :] = near[...]

    @pl.when(jnp.logical_not(even_tile()))
    def _():
        wide[:, :half] = near[...]
        wide[:, half + cols :] = far[...]


def footprint(info, mat):
    width, obs = mat.shape
    local = info[8:9, :].astype(jnp.int32)
    low = local & (GROUP - 1)
    high = lax.shift_right_logical(local, 4)
    rows = lax.broadcasted_iota(jnp.int32, (GROUP, obs), 0)
    offset = (rows - low) & (GROUP - 1)
    piece = jnp.zeros((GROUP, obs), F32)
    for k in range(8):
        piece = piece + jnp.where(offset == k, info[k : k + 1, :], 0.0)
    piece = piece.astype(BF16)
    group = (high + jnp.where(rows < low, 1, 0)).astype(F32).astype(BF16)
    zero = jnp.zeros((GROUP, obs), BF16)
    for g in range(width // GROUP):
        mat[g * GROUP : (g + 1) * GROUP, :] = jnp.where(
            group == jnp.full((GROUP, obs), g, BF16), piece, zero
        )


def slot_weight(info, held):
    slot = info[9:10, :]
    frac = info[10:11, :]
    return jnp.where(slot == held, 1.0 - frac, 0.0) + jnp.where(slot + 1.0 == held, frac, 0.0)


def gather_one(field, info, mat, out):
    chan = out.shape[0]
    own_slot, other_slot = held_slots()
    both = jnp.dot(field, mat[...], preferred_element_type=F32)
    first = slot_weight(info, own_slot)
    second = slot_weight(info, other_slot)
    out[...] = (first * both[:chan] + second * both[chan:]).astype(BF16)


def gather_kernel(mine, other, info, mat, out):
    gather_one(jnp.concatenate([mine[...], other[...]], axis=0), info, mat, out)


def build_gather_kernel(n, mine, other, *refs):
    infos, mats, outs = refs[:n], refs[n : 2 * n], refs[2 * n :]
    field = jnp.concatenate([mine[...], other[...]], axis=0)
    for info, mat, out in zip(infos, mats, outs):
        footprint(info, mat)
        gather_one(field, info, mat, out)


def turn_kernel(source, out):
    out[...] = jnp.transpose(source[...])


def values_kernel(source, inv_var, values, scale, held, sem):
    copy = pltpu.make_async_copy(source, held, sem)
    copy.start()
    scale[...] = jnp.transpose(jnp.broadcast_to(inv_var[...], scale.shape))
    copy.wait()
    values[...] = jnp.transpose(held[...])


def depart_kernel(n, count, *refs):
    parts = refs[:n]
    values, scale, gaps, scaled = refs[n:]
    chan, obs = values.shape
    total = parts[0][...].astype(F32)
    for part in parts[1:]:
        total = total + part[...].astype(F32)
    live = lax.broadcasted_iota(jnp.int32, (chan, obs), 1) < count[0, 0]
    gap = jnp.where(live, values[...] - total, 0.0)
    gaps[...] = gap
    scaled[...] = (gap * scale[:, 0:1]).astype(BF16)


def weighted(info, source, slot):
    return (slot_weight(info, slot) * source[...].astype(F32)).astype(BF16)


def spread_rows(rows, mat):
    return lax.dot_general(
        rows, mat[...], (((1,), (1,)), ((), ())), preferred_element_type=F32
    )


def spread_one(info, source, mat):
    rows = [weighted(info, source, slot) for slot in held_slots()]
    return spread_rows(jnp.concatenate(rows, axis=0), mat)


def spread_first_kernel(info, scaled, mat, acc):
    acc[...] = spread_one(info, scaled, mat)


def spread_next_kernel(before, info, scaled, mat, acc):
    acc[...] = before[...] + spread_one(info, scaled, mat)


def spread_give_kernel(before, info, scaled, mat, give):
    chan = give.shape[0]
    part = spread_rows(weighted(info, scaled, held_slots()[1]), mat)
    give[...] = (before[chan:, :] + part).astype(BF16)


def spread_keep_kernel(before, info, scaled, mat, own):
    chan = own.shape[0]
    own[...] = before[:chan, :] + spread_rows(weighted(info, scaled, held_slots()[0]), mat)


def join_kernel(own, got, mid, near, far):
    cols = mid.shape[1]
    half = cols // 2
    mid[...] = own[:, half : half + cols] + got[:, half : half + cols].astype(F32)
    left = (own[:, :half] + got[:, :half].astype(F32)).astype(BF16)
    right = (own[:, half + cols :] + got[:, half + cols :].astype(F32)).astype(BF16)
    put_rims(near, far, left, right)


def finish_kernel(mid, near, far_even, far_odd, jac, out, rows, sems):
    half = near.shape[1]
    levels = jac.shape[0]
    cut = (levels // 2 + 15) // 16 * 16
    even = even_tile()
    first = mid[:, :half] + jnp.where(even, far_even[...], near[...]).astype(F32)
    last = mid[:, half:] + jnp.where(even, near[...], far_odd[...]).astype(F32)
    total = jnp.concatenate([first, last], axis=1).astype(BF16)
    copies = []
    for index, part in enumerate((slice(0, cut), slice(cut, levels))):
        rows[part, 0, :] = jnp.dot(jac[part, :], total, preferred_element_type=F32)
        copy = pltpu.make_async_copy(rows.at[part], out.at[part], sems.at[index])
        copy.start()
        copies.append(copy)
    for copy in copies:
        copy.wait()


def call(kernel, outs, *args, specs=None, out_specs=None, scratch=(), limit=8 << 20, flops=1 << 20):
    return pl.pallas_call(
        kernel,
        out_shape=[jax.ShapeDtypeStruct(shape, dtype) for shape, dtype in outs],
        in_specs=specs or [VMEM] * len(args),
        out_specs=out_specs or [VMEM] * len(outs),
        scratch_shapes=scratch,
        compiler_params=pltpu.CompilerParams(vmem_limit_bytes=limit),
        cost_estimate=pl.CostEstimate(flops=flops, bytes_accessed=1 << 20, transcendentals=0),
    )(*args)


def make_body(n_tm, n_space):
    lanes = n_tm // 2

    def swap(block, y=0, core=0, tile=None, senders=(0, 1)):
        partner = {
            None: lambda s: s,
            "near": lambda s: s ^ 1,
            "far": lambda s: (s + 1 if s % 2 else s - 1) % n_space,
        }[tile]
        route = []
        for t in range(n_tm):
            for s in range(n_space):
                other = (t // 2 ^ y) * 2 + (t % 2 ^ core)
                if partner(s) % 2 in senders:
                    route.append((other * n_space + partner(s), t * n_space + s))
        return lax.ppermute(block, ("tm", "space"), route)

    def steps(
        state, obs_start, foot_weight, obs_slot, obs_frac, live_count, obs_values, jacobian, inv_var
    ):
        own = state[0]
        cols, levels = own.shape
        half = cols // 2
        width = 2 * cols
        chan = jacobian.shape[1]
        obs = obs_start.shape[0]

        def flat(vector):
            return vector.reshape(1, -1)

        (first,) = call(first_kernel, [((8, 128), F32)], flops=FIRST_FLOPS)
        full, near, far, info = call(
            functools.partial(enter_kernel, n_space),
            [
                ((chan, cols), BF16),
                ((chan, half), BF16),
                ((chan, half), BF16),
                ((16, obs), F32),
            ],
            first,
            own.T,
            jacobian,
            flat(obs_start),
            foot_weight.T,
            flat(obs_slot),
            flat(obs_frac),
        )
        near, far = swap(near, tile="near"), swap(far, tile="far")
        infos = [info] + [swap(info, y=j) for j in range(1, lanes)]
        (wide,) = call(widen_kernel, [((chan, width), BF16)], full, near, far)
        other = swap(wide, core=1)
        mats = [None] * lanes
        (mats[2],) = call(footprint, [((width, obs), BF16)], infos[2])

        def gather(which):
            outs = call(
                functools.partial(build_gather_kernel, len(which)),
                [((width, obs), BF16)] * len(which) + [((chan, obs), BF16)] * len(which),
                wide,
                other,
                *[infos[j] for j in which],
            )
            for index, j in enumerate(which):
                mats[j] = outs[index]
            return outs[len(which) :]

        (far,) = call(gather_kernel, [((chan, obs), BF16)], wide, other, infos[2], mats[2])
        parts = [None] * lanes
        parts[2] = swap(far, y=2)
        for j in SWAP_ORDER[1:]:
            (part,) = gather([j])
            parts[j] = swap(part, y=j)
        (parts[0],) = gather([0])
        values, scale = call(
            values_kernel,
            [((chan, obs), F32), ((chan, chan), F32)],
            obs_values,
            flat(inv_var),
            specs=[HBM, VMEM],
            scratch=[pltpu.VMEM((obs, chan), F32), pltpu.SemaphoreType.DMA],
        )
        gaps, scaled = call(
            functools.partial(depart_kernel, lanes),
            [((chan, obs), F32), ((chan, obs), BF16)],
            live_count,
            *parts,
            values,
            scale,
            specs=[SMEM] + [VMEM] * (lanes + 2),
        )
        all_scaled = [scaled] + [swap(scaled, y=j) for j in range(1, lanes)]
        (acc,) = call(spread_first_kernel, [((2 * chan, width), F32)], info, scaled, mats[0])
        (departures,) = call(turn_kernel, [((obs, chan), F32)], gaps)
        *early, last = SWAP_ORDER
        for j in early:
            (acc,) = call(
                spread_next_kernel,
                [((2 * chan, width), F32)],
                acc,
                infos[j],
                all_scaled[j],
                mats[j],
            )
        rest = (acc, infos[last], all_scaled[last], mats[last])
        (give,) = call(spread_give_kernel, [((chan, width), BF16)], *rest)
        give = swap(give, core=1)
        (mine,) = call(spread_keep_kernel, [((chan, width), F32)], *rest)
        mid, near, far = call(
            join_kernel, [((chan, cols), F32)] + [((chan, half), BF16)] * 2, mine, give
        )
        (adjoint,) = call(
            finish_kernel,
            [((levels, 1, cols), F32)],
            mid,
            swap(near, tile="near"),
            swap(far, tile="far", senders=(1,)),
            swap(far, tile="far", senders=(0,)),
            jacobian,
            out_specs=[HBM],
            scratch=[pltpu.VMEM((levels, 1, cols), F32), pltpu.SemaphoreType.DMA((2,))],
        )
        return (departures, jnp.transpose(adjoint, (1, 2, 0)))

    return steps


def solution(mesh):
    return jax.shard_map(
        make_body(mesh.shape["tm"], mesh.shape["space"]),
        mesh=mesh,
        in_specs=(
            P("tm", "space", None),
            P(("tm", "space")),
            P(("tm", "space"), None),
            P(("tm", "space")),
            P(("tm", "space")),
            P("tm", "space"),
            P(("tm", "space"), None),
            P(),
            P(),
        ),
        out_specs=(P(("tm", "space"), None), P("tm", "space", None)),
        check_vma=False,
    )
```

```python
import functools

import jax
import jax.numpy as jnp
from jax import lax
from jax.experimental import pallas as pl
from jax.experimental.pallas import tpu as pltpu
from jax.sharding import PartitionSpec as P


F32 = jnp.float32
BF16 = jnp.bfloat16
GROUP = 16
SWAP_ORDER = (2, 3, 1)
LAND_ORDER = (2, 1, 3)
FIRST_FLOPS = 1 << 34


VMEM = pl.BlockSpec(memory_space=pltpu.VMEM)
SMEM = pl.BlockSpec(memory_space=pltpu.SMEM)
HBM = pl.BlockSpec(memory_space=pltpu.HBM)


def held_slots():
    turn = lax.axis_index("tm")
    return turn.astype(F32), (turn ^ 1).astype(F32)


def even_tile():
    return lax.axis_index("space") % 2 == 0


def put_rims(near, far, left, right):
    @pl.when(even_tile())
    def _():
        near[...] = right
        far[...] = left

    @pl.when(jnp.logical_not(even_tile()))
    def _():
        near[...] = left
        far[...] = right


def first_kernel(out):
    out[...] = jnp.zeros_like(out)


def enter_kernel(tiles, first, state, jac, start, weight, slot, frac, full, near, far, info):
    cols = full.shape[1]
    half = cols // 2
    out = lax.dot_general(
        jac[...], state[...], (((0,), (0,)), ((), ())), preferred_element_type=F32
    ).astype(BF16)
    full[...] = out
    put_rims(near, far, out[:, :half], out[:, half:])
    base = lax.axis_index("space") * cols - half
    total = cols * tiles
    local = start[...] - base
    local = jnp.where(local < 0, local + total, local)
    local = jnp.where(local >= total, local - total, local)
    rows = lax.broadcasted_iota(jnp.int32, (8, local.shape[1]), 0)
    extra = jnp.where(rows == 0, local.astype(F32), 0.0)
    extra = jnp.where(rows == 1, slot[...].astype(F32), extra)
    extra = jnp.where(rows == 2, frac[...], extra)
    info[0:8, :] = weight[...].astype(F32)
    info[8:16, :] = extra


def widen_kernel(full, near, far, wide):
    cols = full.shape[1]
    half = cols // 2
    wide[:, half : half + cols] = full[...]

    @pl.when(even_tile())
    def _():
        wide[:, :half] = far[...]
        wide[:, half + cols :] = near[...]

    @pl.when(jnp.logical_not(even_tile()))
    def _():
        wide[:, :half] = near[...]
        wide[:, half + cols :] = far[...]


def footprint(info, mat):
    width, obs = mat.shape
    local = info[8:9, :].astype(jnp.int32)
    low = local & (GROUP - 1)
    high = lax.shift_right_logical(local, 4)
    rows = lax.broadcasted_iota(jnp.int32, (GROUP, obs), 0)
    offset = (rows - low) & (GROUP - 1)
    piece = jnp.zeros((GROUP, obs), F32)
    for k in range(8):
        piece = piece + jnp.where(offset == k, info[k : k + 1, :], 0.0)
    piece = piece.astype(BF16)
    group = (high + jnp.where(rows < low, 1, 0)).astype(F32).astype(BF16)
    zero = jnp.zeros((GROUP, obs), BF16)
    for g in range(width // GROUP):
        mat[g * GROUP : (g + 1) * GROUP, :] = jnp.where(
            group == jnp.full((GROUP, obs), g, BF16), piece, zero
        )


def slot_weight(info, held):
    slot = info[9:10, :]
    frac = info[10:11, :]
    return jnp.where(slot == held, 1.0 - frac, 0.0) + jnp.where(slot + 1.0 == held, frac, 0.0)


def gather_one(field, info, mat, out):
    chan = out.shape[0]
    own_slot, other_slot = held_slots()
    both = jnp.dot(field, mat[...], preferred_element_type=F32)
    first = slot_weight(info, own_slot)
    second = slot_weight(info, other_slot)
    out[...] = (first * both[:chan] + second * both[chan:]).astype(BF16)


def gather_kernel(mine, other, info, mat, out):
    gather_one(jnp.concatenate([mine[...], other[...]], axis=0), info, mat, out)


def build_gather_kernel(n, mine, other, *refs):
    infos, mats, outs = refs[:n], refs[n : 2 * n], refs[2 * n :]
    field = jnp.concatenate([mine[...], other[...]], axis=0)
    for info, mat, out in zip(infos, mats, outs):
        footprint(info, mat)
        gather_one(field, info, mat, out)


def turn_kernel(source, out):
    out[...] = jnp.transpose(source[...])


def values_kernel(source, inv_var, values, scale, held, sem):
    copy = pltpu.make_async_copy(source, held, sem)
    copy.start()
    scale[...] = jnp.transpose(jnp.broadcast_to(inv_var[...], scale.shape))
    copy.wait()
    values[...] = jnp.transpose(held[...])


def depart_kernel(n, count, *refs):
    parts = refs[:n]
    values, scale, gaps, scaled = refs[n:]
    chan, obs = values.shape
    total = parts[0][...].astype(F32)
    for part in parts[1:]:
        total = total + part[...].astype(F32)
    live = lax.broadcasted_iota(jnp.int32, (chan, obs), 1) < count[0, 0]
    gap = jnp.where(live, values[...] - total, 0.0)
    gaps[...] = gap
    scaled[...] = (gap * scale[:, 0:1]).astype(BF16)


def weighted(info, source, slot):
    return (slot_weight(info, slot) * source[...].astype(F32)).astype(BF16)


def spread_rows(rows, mat):
    return lax.dot_general(
        rows, mat[...], (((1,), (1,)), ((), ())), preferred_element_type=F32
    )


def spread_one(info, source, mat):
    rows = [weighted(info, source, slot) for slot in held_slots()]
    return spread_rows(jnp.concatenate(rows, axis=0), mat)


def spread_first_kernel(info, scaled, mat, acc):
    acc[...] = spread_one(info, scaled, mat)


def spread_next_kernel(before, info, scaled, mat, acc):
    acc[...] = before[...] + spread_one(info, scaled, mat)


def spread_give_kernel(before, info, scaled, mat, give):
    chan = give.shape[0]
    part = spread_rows(weighted(info, scaled, held_slots()[1]), mat)
    give[...] = (before[chan:, :] + part).astype(BF16)


def spread_keep_kernel(before, info, scaled, mat, own):
    chan = own.shape[0]
    own[...] = before[:chan, :] + spread_rows(weighted(info, scaled, held_slots()[0]), mat)


def join_kernel(own, got, mid, near, far):
    cols = mid.shape[1]
    half = cols // 2
    mid[...] = own[:, half : half + cols] + got[:, half : half + cols].astype(F32)
    left = (own[:, :half] + got[:, :half].astype(F32)).astype(BF16)
    right = (own[:, half + cols :] + got[:, half + cols :].astype(F32)).astype(BF16)
    put_rims(near, far, left, right)


def finish_kernel(mid, near, far, jac, out, rows, sems):
    half = near.shape[1]
    levels = jac.shape[0]
    cut = (levels // 2 + 15) // 16 * 16
    even = even_tile()
    first = mid[:, :half] + jnp.where(even, far[...], near[...]).astype(F32)
    last = mid[:, half:] + jnp.where(even, near[...], far[...]).astype(F32)
    total = jnp.concatenate([first, last], axis=1).astype(BF16)
    copies = []
    for index, part in enumerate((slice(0, cut), slice(cut, levels))):
        rows[part, 0, :] = jnp.dot(jac[part, :], total, preferred_element_type=F32)
        copy = pltpu.make_async_copy(rows.at[part], out.at[part], sems.at[index])
        copy.start()
        copies.append(copy)
    for copy in copies:
        copy.wait()


def call(kernel, outs, *args, specs=None, out_specs=None, scratch=(), limit=8 << 20, flops=1 << 20):
    return pl.pallas_call(
        kernel,
        out_shape=[jax.ShapeDtypeStruct(shape, dtype) for shape, dtype in outs],
        in_specs=specs or [VMEM] * len(args),
        out_specs=out_specs or [VMEM] * len(outs),
        scratch_shapes=scratch,
        compiler_params=pltpu.CompilerParams(vmem_limit_bytes=limit),
        cost_estimate=pl.CostEstimate(flops=flops, bytes_accessed=1 << 20, transcendentals=0),
    )(*args)


def make_body(n_tm, n_space):
    lanes = n_tm // 2

    def swap(block, y=0, core=0, tile=None):
        partner = {
            None: lambda s: s,
            "near": lambda s: s ^ 1,
            "far": lambda s: (s + 1 if s % 2 else s - 1) % n_space,
        }[tile]
        route = []
        for t in range(n_tm):
            for s in range(n_space):
                other = (t // 2 ^ y) * 2 + (t % 2 ^ core)
                route.append((other * n_space + partner(s), t * n_space + s))
        return lax.ppermute(block, ("tm", "space"), route)

    def steps(
        state, obs_start, foot_weight, obs_slot, obs_frac, live_count, obs_values, jacobian, inv_var
    ):
        own = state[0]
        cols, levels = own.shape
        half = cols // 2
        width = 2 * cols
        chan = jacobian.shape[1]
        obs = obs_start.shape[0]

        def flat(vector):
            return vector.reshape(1, -1)

        (first,) = call(first_kernel, [((8, 128), F32)], flops=FIRST_FLOPS)
        full, near, far, info = call(
            functools.partial(enter_kernel, n_space),
            [
                ((chan, cols), BF16),
                ((chan, half), BF16),
                ((chan, half), BF16),
                ((16, obs), F32),
            ],
            first,
            own.T,
            jacobian,
            flat(obs_start),
            foot_weight.T,
            flat(obs_slot),
            flat(obs_frac),
        )
        near, far = swap(near, tile="near"), swap(far, tile="far")
        infos = [info] + [swap(info, y=j) for j in range(1, lanes)]
        (wide,) = call(widen_kernel, [((chan, width), BF16)], full, near, far)
        other = swap(wide, core=1)
        mats = [None] * lanes
        (mats[2],) = call(footprint, [((width, obs), BF16)], infos[2])

        def gather(which):
            outs = call(
                functools.partial(build_gather_kernel, len(which)),
                [((width, obs), BF16)] * len(which) + [((chan, obs), BF16)] * len(which),
                wide,
                other,
                *[infos[j] for j in which],
            )
            for index, j in enumerate(which):
                mats[j] = outs[index]
            return outs[len(which) :]

        (far,) = call(gather_kernel, [((chan, obs), BF16)], wide, other, infos[2], mats[2])
        parts = [None] * lanes
        parts[2] = swap(far, y=2)
        for j in SWAP_ORDER[1:]:
            (part,) = gather([j])
            parts[j] = swap(part, y=j)
        (parts[0],) = gather([0])
        values, scale = call(
            values_kernel,
            [((chan, obs), F32), ((chan, chan), F32)],
            obs_values,
            flat(inv_var),
            specs=[HBM, VMEM],
            scratch=[pltpu.VMEM((obs, chan), F32), pltpu.SemaphoreType.DMA],
        )
        gaps, scaled = call(
            functools.partial(depart_kernel, lanes),
            [((chan, obs), F32), ((chan, obs), BF16)],
            live_count,
            *parts,
            values,
            scale,
            specs=[SMEM] + [VMEM] * (lanes + 2),
        )
        all_scaled = [scaled] + [swap(scaled, y=j) for j in range(1, lanes)]
        (acc,) = call(spread_first_kernel, [((2 * chan, width), F32)], info, scaled, mats[0])
        (departures,) = call(turn_kernel, [((obs, chan), F32)], gaps)
        *early, last = LAND_ORDER
        for j in early:
            (acc,) = call(
                spread_next_kernel,
                [((2 * chan, width), F32)],
                acc,
                infos[j],
                all_scaled[j],
                mats[j],
            )
        rest = (acc, infos[last], all_scaled[last], mats[last])
        (give,) = call(spread_give_kernel, [((chan, width), BF16)], *rest)
        give = swap(give, core=1)
        (mine,) = call(spread_keep_kernel, [((chan, width), F32)], *rest)
        mid, near, far = call(
            join_kernel, [((chan, cols), F32)] + [((chan, half), BF16)] * 2, mine, give
        )
        (adjoint,) = call(
            finish_kernel,
            [((levels, 1, cols), F32)],
            mid,
            swap(near, tile="near"),
            swap(far, tile="far"),
            jacobian,
            out_specs=[HBM],
            scratch=[pltpu.VMEM((levels, 1, cols), F32), pltpu.SemaphoreType.DMA((2,))],
        )
        return (departures, jnp.transpose(adjoint, (1, 2, 0)))

    return steps


def solution(mesh):
    return jax.shard_map(
        make_body(mesh.shape["tm"], mesh.shape["space"]),
        mesh=mesh,
        in_specs=(
            P("tm", "space", None),
            P(("tm", "space")),
            P(("tm", "space"), None),
            P(("tm", "space")),
            P(("tm", "space")),
            P("tm", "space"),
            P(("tm", "space"), None),
            P(),
            P(),
        ),
        out_specs=(P(("tm", "space"), None), P("tm", "space", None)),
        check_vma=False,
    )
```

```python
import functools

import jax
import jax.numpy as jnp
from jax import lax
from jax.experimental import pallas as pl
from jax.experimental.pallas import tpu as pltpu
from jax.sharding import PartitionSpec as P


F32 = jnp.float32
BF16 = jnp.bfloat16
GROUP = 16
SWAP_ORDER = (2, 3, 1)
LAND_ORDER = (2, 1, 3)
FIRST_FLOPS = 1 << 34


VMEM = pl.BlockSpec(memory_space=pltpu.VMEM)
SMEM = pl.BlockSpec(memory_space=pltpu.SMEM)
HBM = pl.BlockSpec(memory_space=pltpu.HBM)


def held_slots():
    turn = lax.axis_index("tm")
    return turn.astype(F32), (turn ^ 1).astype(F32)


def even_tile():
    return lax.axis_index("space") % 2 == 0


def put_rims(near, far, left, right):
    @pl.when(even_tile())
    def _():
        near[...] = right
        far[...] = left

    @pl.when(jnp.logical_not(even_tile()))
    def _():
        near[...] = left
        far[...] = right


def first_kernel(out):
    out[...] = jnp.zeros_like(out)


def enter_kernel(tiles, first, state, jac, start, weight, slot, frac, full, near, far, info):
    cols = full.shape[1]
    half = cols // 2
    out = lax.dot_general(
        jac[...], state[...], (((0,), (0,)), ((), ())), preferred_element_type=F32
    ).astype(BF16)
    full[...] = out
    put_rims(near, far, out[:, :half], out[:, half:])
    base = lax.axis_index("space") * cols - half
    total = cols * tiles
    local = start[...] - base
    local = jnp.where(local < 0, local + total, local)
    local = jnp.where(local >= total, local - total, local)
    rows = lax.broadcasted_iota(jnp.int32, (8, local.shape[1]), 0)
    extra = jnp.where(rows == 0, local.astype(F32), 0.0)
    extra = jnp.where(rows == 1, slot[...].astype(F32), extra)
    extra = jnp.where(rows == 2, frac[...], extra)
    info[0:8, :] = weight[...].astype(F32)
    info[8:16, :] = extra


def pair_kernel(own, got, pair):
    rows = own.shape[0]
    pair[:rows, :] = own[...]
    pair[rows:, :] = got[...]


def widen_kernel(full, near, far, wide):
    cols = full.shape[1]
    half = cols // 2
    wide[:, half : half + cols] = full[...]

    @pl.when(even_tile())
    def _():
        wide[:, :half] = far[...]
        wide[:, half + cols :] = near[...]

    @pl.when(jnp.logical_not(even_tile()))
    def _():
        wide[:, :half] = near[...]
        wide[:, half + cols :] = far[...]


def footprint(info, mat):
    width, obs = mat.shape
    local = info[8:9, :].astype(jnp.int32)
    low = local & (GROUP - 1)
    high = lax.shift_right_logical(local, 4)
    rows = lax.broadcasted_iota(jnp.int32, (GROUP, obs), 0)
    offset = (rows - low) & (GROUP - 1)
    piece = jnp.zeros((GROUP, obs), F32)
    for k in range(8):
        piece = piece + jnp.where(offset == k, info[k : k + 1, :], 0.0)
    piece = piece.astype(BF16)
    group = (high + jnp.where(rows < low, 1, 0)).astype(F32).astype(BF16)
    zero = jnp.zeros((GROUP, obs), BF16)
    for g in range(width // GROUP):
        mat[g * GROUP : (g + 1) * GROUP, :] = jnp.where(
            group == jnp.full((GROUP, obs), g, BF16), piece, zero
        )


def slot_weight(info, held):
    slot = info[9:10, :]
    frac = info[10:11, :]
    return jnp.where(slot == held, 1.0 - frac, 0.0) + jnp.where(slot + 1.0 == held, frac, 0.0)


def gather_one(field, info, mat, out):
    chan = out.shape[0]
    own_slot, other_slot = held_slots()
    both = jnp.dot(field, mat[...], preferred_element_type=F32)
    first = slot_weight(info, own_slot)
    second = slot_weight(info, other_slot)
    out[...] = (first * both[:chan] + second * both[chan:]).astype(BF16)


def gather_kernel(mine, other, info, mat, out):
    gather_one(jnp.concatenate([mine[...], other[...]], axis=0), info, mat, out)


def build_gather_kernel(n, mine, other, *refs):
    infos, mats, outs = refs[:n], refs[n : 2 * n], refs[2 * n :]
    field = jnp.concatenate([mine[...], other[...]], axis=0)
    for info, mat, out in zip(infos, mats, outs):
        footprint(info, mat)
        gather_one(field, info, mat, out)


def turn_kernel(source, out):
    out[...] = jnp.transpose(source[...])


def values_kernel(source, inv_var, values, scale, held, sem):
    copy = pltpu.make_async_copy(source, held, sem)
    copy.start()
    scale[...] = jnp.transpose(jnp.broadcast_to(inv_var[...], scale.shape))
    copy.wait()
    values[...] = jnp.transpose(held[...])


def depart_kernel(n, count, *refs):
    parts = refs[:n]
    values, scale, gaps, scaled = refs[n:]
    chan, obs = values.shape
    total = parts[0][...].astype(F32)
    for part in parts[1:]:
        total = total + part[...].astype(F32)
    live = lax.broadcasted_iota(jnp.int32, (chan, obs), 1) < count[0, 0]
    gap = jnp.where(live, values[...] - total, 0.0)
    gaps[...] = gap
    scaled[...] = (gap * scale[:, 0:1]).astype(BF16)


def weighted(info, source, slot):
    return (slot_weight(info, slot) * source[...].astype(F32)).astype(BF16)


def spread_rows(rows, mat):
    return lax.dot_general(
        rows, mat[...], (((1,), (1,)), ((), ())), preferred_element_type=F32
    )


def spread_one(info, source, mat):
    rows = [weighted(info, source, slot) for slot in held_slots()]
    return spread_rows(jnp.concatenate(rows, axis=0), mat)


def spread_first_kernel(info, scaled, mat, acc):
    acc[...] = spread_one(info, scaled, mat)


def spread_next_kernel(before, info, scaled, mat, acc):
    acc[...] = before[...] + spread_one(info, scaled, mat)


def spread_give_kernel(before, info, scaled, mat, give):
    chan = give.shape[0]
    part = spread_rows(weighted(info, scaled, held_slots()[1]), mat)
    give[...] = (before[chan:, :] + part).astype(BF16)


def spread_keep_kernel(before, info, scaled, mat, own):
    chan = own.shape[0]
    own[...] = before[:chan, :] + spread_rows(weighted(info, scaled, held_slots()[0]), mat)


def join_kernel(own, got, mid, near, far):
    cols = mid.shape[1]
    half = cols // 2
    mid[...] = own[:, half : half + cols] + got[:, half : half + cols].astype(F32)
    left = (own[:, :half] + got[:, :half].astype(F32)).astype(BF16)
    right = (own[:, half + cols :] + got[:, half + cols :].astype(F32)).astype(BF16)
    put_rims(near, far, left, right)


def finish_kernel(mid, near, far, jac, out, rows, sems):
    half = near.shape[1]
    levels = jac.shape[0]
    cut = (levels // 2 + 15) // 16 * 16
    even = even_tile()
    first = mid[:, :half] + jnp.where(even, far[...], near[...]).astype(F32)
    last = mid[:, half:] + jnp.where(even, near[...], far[...]).astype(F32)
    total = jnp.concatenate([first, last], axis=1).astype(BF16)
    copies = []
    for index, part in enumerate((slice(0, cut), slice(cut, levels))):
        rows[part, 0, :] = jnp.dot(jac[part, :], total, preferred_element_type=F32)
        copy = pltpu.make_async_copy(rows.at[part], out.at[part], sems.at[index])
        copy.start()
        copies.append(copy)
    for copy in copies:
        copy.wait()


def call(kernel, outs, *args, specs=None, out_specs=None, scratch=(), limit=8 << 20, flops=1 << 20):
    return pl.pallas_call(
        kernel,
        out_shape=[jax.ShapeDtypeStruct(shape, dtype) for shape, dtype in outs],
        in_specs=specs or [VMEM] * len(args),
        out_specs=out_specs or [VMEM] * len(outs),
        scratch_shapes=scratch,
        compiler_params=pltpu.CompilerParams(vmem_limit_bytes=limit),
        cost_estimate=pl.CostEstimate(flops=flops, bytes_accessed=1 << 20, transcendentals=0),
    )(*args)


def make_body(n_tm, n_space):
    lanes = n_tm // 2

    def swap(block, y=0, core=0, tile=None):
        partner = {
            None: lambda s: s,
            "near": lambda s: s ^ 1,
            "far": lambda s: (s + 1 if s % 2 else s - 1) % n_space,
        }[tile]
        route = []
        for t in range(n_tm):
            for s in range(n_space):
                other = (t // 2 ^ y) * 2 + (t % 2 ^ core)
                route.append((other * n_space + partner(s), t * n_space + s))
        return lax.ppermute(block, ("tm", "space"), route)

    def steps(
        state, obs_start, foot_weight, obs_slot, obs_frac, live_count, obs_values, jacobian, inv_var
    ):
        own = state[0]
        cols, levels = own.shape
        half = cols // 2
        width = 2 * cols
        chan = jacobian.shape[1]
        obs = obs_start.shape[0]

        def flat(vector):
            return vector.reshape(1, -1)

        (first,) = call(first_kernel, [((8, 128), F32)], flops=FIRST_FLOPS)
        full, near, far, info = call(
            functools.partial(enter_kernel, n_space),
            [
                ((chan, cols), BF16),
                ((chan, half), BF16),
                ((chan, half), BF16),
                ((16, obs), F32),
            ],
            first,
            own.T,
            jacobian,
            flat(obs_start),
            foot_weight.T,
            flat(obs_slot),
            flat(obs_frac),
        )
        near, far = swap(near, tile="near"), swap(far, tile="far")
        got = swap(info, y=2)
        (pair,) = call(pair_kernel, [((32, obs), F32)], info, got)
        pair = swap(pair, y=1)
        infos = [info, pair[:16], got, pair[16:]]
        (wide,) = call(widen_kernel, [((chan, width), BF16)], full, near, far)
        other = swap(wide, core=1)
        mats = [None] * lanes
        (mats[2],) = call(footprint, [((width, obs), BF16)], infos[2])

        def gather(which):
            outs = call(
                functools.partial(build_gather_kernel, len(which)),
                [((width, obs), BF16)] * len(which) + [((chan, obs), BF16)] * len(which),
                wide,
                other,
                *[infos[j] for j in which],
            )
            for index, j in enumerate(which):
                mats[j] = outs[index]
            return outs[len(which) :]

        (far,) = call(gather_kernel, [((chan, obs), BF16)], wide, other, infos[2], mats[2])
        parts = [None] * lanes
        parts[2] = swap(far, y=2)
        for j in SWAP_ORDER[1:]:
            (part,) = gather([j])
            parts[j] = swap(part, y=j)
        (parts[0],) = gather([0])
        values, scale = call(
            values_kernel,
            [((chan, obs), F32), ((chan, chan), F32)],
            obs_values,
            flat(inv_var),
            specs=[HBM, VMEM],
            scratch=[pltpu.VMEM((obs, chan), F32), pltpu.SemaphoreType.DMA],
        )
        gaps, scaled = call(
            functools.partial(depart_kernel, lanes),
            [((chan, obs), F32), ((chan, obs), BF16)],
            live_count,
            *parts,
            values,
            scale,
            specs=[SMEM] + [VMEM] * (lanes + 2),
        )
        all_scaled = [scaled] + [swap(scaled, y=j) for j in range(1, lanes)]
        (acc,) = call(spread_first_kernel, [((2 * chan, width), F32)], info, scaled, mats[0])
        (departures,) = call(turn_kernel, [((obs, chan), F32)], gaps)
        *early, last = LAND_ORDER
        for j in early:
            (acc,) = call(
                spread_next_kernel,
                [((2 * chan, width), F32)],
                acc,
                infos[j],
                all_scaled[j],
                mats[j],
            )
        rest = (acc, infos[last], all_scaled[last], mats[last])
        (give,) = call(spread_give_kernel, [((chan, width), BF16)], *rest)
        give = swap(give, core=1)
        (mine,) = call(spread_keep_kernel, [((chan, width), F32)], *rest)
        mid, near, far = call(
            join_kernel, [((chan, cols), F32)] + [((chan, half), BF16)] * 2, mine, give
        )
        (adjoint,) = call(
            finish_kernel,
            [((levels, 1, cols), F32)],
            mid,
            swap(near, tile="near"),
            swap(far, tile="far"),
            jacobian,
            out_specs=[HBM],
            scratch=[pltpu.VMEM((levels, 1, cols), F32), pltpu.SemaphoreType.DMA((2,))],
        )
        return (departures, jnp.transpose(adjoint, (1, 2, 0)))

    return steps


def solution(mesh):
    return jax.shard_map(
        make_body(mesh.shape["tm"], mesh.shape["space"]),
        mesh=mesh,
        in_specs=(
            P("tm", "space", None),
            P(("tm", "space")),
            P(("tm", "space"), None),
            P(("tm", "space")),
            P(("tm", "space")),
            P("tm", "space"),
            P(("tm", "space"), None),
            P(),
            P(),
        ),
        out_specs=(P(("tm", "space"), None), P("tm", "space", None)),
        check_vma=False,
    )
```

```python
import functools

import jax
import jax.numpy as jnp
from jax import lax
from jax.experimental import pallas as pl
from jax.experimental.pallas import tpu as pltpu
from jax.sharding import PartitionSpec as P


F32 = jnp.float32
BF16 = jnp.bfloat16
GROUP = 16
PIECE = 32
SWAP_ORDER = (2, 3, 1)
LAND_ORDER = (2, 1, 3)
FIRST_FLOPS = 1 << 34


VMEM = pl.BlockSpec(memory_space=pltpu.VMEM)
SMEM = pl.BlockSpec(memory_space=pltpu.SMEM)
HBM = pl.BlockSpec(memory_space=pltpu.HBM)


def held_slots():
    turn = lax.axis_index("tm")
    return turn.astype(F32), (turn ^ 1).astype(F32)


def even_tile():
    return lax.axis_index("space") % 2 == 0


def put_rims(near, far, left, right):
    @pl.when(even_tile())
    def _():
        near[...] = right
        far[...] = left

    @pl.when(jnp.logical_not(even_tile()))
    def _():
        near[...] = left
        far[...] = right


def first_kernel(out):
    out[...] = jnp.zeros_like(out)


def enter_kernel(tiles, first, state, jac, start, weight, slot, frac, full, near, far, info):
    cols = full.shape[1]
    half = cols // 2
    out = lax.dot_general(
        jac[...], state[...], (((0,), (0,)), ((), ())), preferred_element_type=F32
    ).astype(BF16)
    full[...] = out
    put_rims(near, far, out[:, :half], out[:, half:])
    base = lax.axis_index("space") * cols - half
    total = cols * tiles
    local = start[...] - base
    local = jnp.where(local < 0, local + total, local)
    local = jnp.where(local >= total, local - total, local)
    rows = lax.broadcasted_iota(jnp.int32, (8, local.shape[1]), 0)
    extra = jnp.where(rows == 0, local.astype(F32), 0.0)
    extra = jnp.where(rows == 1, slot[...].astype(F32), extra)
    extra = jnp.where(rows == 2, frac[...], extra)
    info[0:8, :] = weight[...].astype(F32)
    info[8:16, :] = extra


def widen_kernel(full, near, far, wide):
    cols = full.shape[1]
    half = cols // 2
    wide[:, half : half + cols] = full[...]

    @pl.when(even_tile())
    def _():
        wide[:, :half] = far[...]
        wide[:, half + cols :] = near[...]

    @pl.when(jnp.logical_not(even_tile()))
    def _():
        wide[:, :half] = near[...]
        wide[:, half + cols :] = far[...]


def footprint(info, mat):
    width, obs = mat.shape
    local = info[8:9, :].astype(jnp.int32)
    low = local & (GROUP - 1)
    high = lax.shift_right_logical(local, 4)
    rows = lax.broadcasted_iota(jnp.int32, (GROUP, obs), 0)
    offset = (rows - low) & (GROUP - 1)
    piece = jnp.zeros((GROUP, obs), F32)
    for k in range(8):
        piece = piece + jnp.where(offset == k, info[k : k + 1, :], 0.0)
    piece = piece.astype(BF16)
    group = (high + jnp.where(rows < low, 1, 0)).astype(F32).astype(BF16)
    zero = jnp.zeros((GROUP, obs), BF16)
    for g in range(width // GROUP):
        mat[g * GROUP : (g + 1) * GROUP, :] = jnp.where(
            group == jnp.full((GROUP, obs), g, BF16), piece, zero
        )


def slot_weight(info, held):
    slot = info[9:10, :]
    frac = info[10:11, :]
    return jnp.where(slot == held, 1.0 - frac, 0.0) + jnp.where(slot + 1.0 == held, frac, 0.0)


def gather_one(field, info, mat, out):
    chan = out.shape[0]
    own_slot, other_slot = held_slots()
    both = jnp.dot(field, mat[...], preferred_element_type=F32)
    first = slot_weight(info, own_slot)
    second = slot_weight(info, other_slot)
    out[...] = (first * both[:chan] + second * both[chan:]).astype(BF16)


def gather_kernel(mine, other, info, mat, out):
    gather_one(jnp.concatenate([mine[...], other[...]], axis=0), info, mat, out)


def build_gather_kernel(n, mine, other, *refs):
    infos, mats, outs = refs[:n], refs[n : 2 * n], refs[2 * n :]
    field = jnp.concatenate([mine[...], other[...]], axis=0)
    for info, mat, out in zip(infos, mats, outs):
        footprint(info, mat)
        gather_one(field, info, mat, out)


def turn_kernel(source, out):
    out[...] = jnp.transpose(source[...])


def values_kernel(source, inv_var, values, scale, held, sem):
    copy = pltpu.make_async_copy(source, held, sem)
    copy.start()
    scale[...] = jnp.transpose(jnp.broadcast_to(inv_var[...], scale.shape))
    copy.wait()
    values[...] = jnp.transpose(held[...])


def depart_kernel(n, count, *refs):
    parts = refs[:n]
    values, scale, gaps, scaled = refs[n:]
    chan, obs = values.shape
    total = parts[0][...].astype(F32)
    for part in parts[1:]:
        total = total + part[...].astype(F32)
    live = lax.broadcasted_iota(jnp.int32, (chan, obs), 1) < count[0, 0]
    gap = jnp.where(live, values[...] - total, 0.0)
    gaps[...] = gap
    scaled[...] = (gap * scale[:, 0:1]).astype(BF16)


def weighted(info, source, slot):
    return (slot_weight(info, slot) * source[...].astype(F32)).astype(BF16)


def spread_rows(rows, mat):
    return lax.dot_general(
        rows, mat[...], (((1,), (1,)), ((), ())), preferred_element_type=F32
    )


def spread_one(info, source, mat):
    rows = [weighted(info, source, slot) for slot in held_slots()]
    return spread_rows(jnp.concatenate(rows, axis=0), mat)


def spread_first_kernel(info, scaled, mat, acc):
    acc[...] = spread_one(info, scaled, mat)


def spread_next_kernel(before, info, scaled, mat, acc):
    acc[...] = before[...] + spread_one(info, scaled, mat)


def spread_give_kernel(before, info, scaled, mat, give):
    chan = give.shape[0]
    part = spread_rows(weighted(info, scaled, held_slots()[1]), mat)
    give[...] = (before[chan:, :] + part).astype(BF16)


def spread_keep_kernel(before, info, scaled, mat, own):
    chan = own.shape[0]
    own[...] = before[:chan, :] + spread_rows(weighted(info, scaled, held_slots()[0]), mat)


def join_kernel(own, got, mid, near, far):
    cols = mid.shape[1]
    half = cols // 2
    mid[...] = own[:, half : half + cols] + got[:, half : half + cols].astype(F32)
    left = (own[:, :half] + got[:, :half].astype(F32)).astype(BF16)
    right = (own[:, half + cols :] + got[:, half + cols :].astype(F32)).astype(BF16)
    put_rims(near, far, left, right)


def finish_kernel(mid, near, far, jac, out, rows, sems):
    half = near.shape[1]
    levels = jac.shape[0]
    even = even_tile()
    first = mid[:, :half] + jnp.where(even, far[...], near[...]).astype(F32)
    last = mid[:, half:] + jnp.where(even, near[...], far[...]).astype(F32)
    total = jnp.concatenate([first, last], axis=1).astype(BF16)
    copies = []
    for index, begin in enumerate(range(0, levels, PIECE)):
        part = slice(begin, min(begin + PIECE, levels))
        rows[part, 0, :] = jnp.dot(jac[part, :], total, preferred_element_type=F32)
        copy = pltpu.make_async_copy(rows.at[part], out.at[part], sems.at[index])
        copy.start()
        copies.append(copy)
    for copy in copies:
        copy.wait()


def call(kernel, outs, *args, specs=None, out_specs=None, scratch=(), limit=8 << 20, flops=1 << 20):
    return pl.pallas_call(
        kernel,
        out_shape=[jax.ShapeDtypeStruct(shape, dtype) for shape, dtype in outs],
        in_specs=specs or [VMEM] * len(args),
        out_specs=out_specs or [VMEM] * len(outs),
        scratch_shapes=scratch,
        compiler_params=pltpu.CompilerParams(vmem_limit_bytes=limit),
        cost_estimate=pl.CostEstimate(flops=flops, bytes_accessed=1 << 20, transcendentals=0),
    )(*args)


def make_body(n_tm, n_space):
    lanes = n_tm // 2

    def swap(block, y=0, core=0, tile=None):
        partner = {
            None: lambda s: s,
            "near": lambda s: s ^ 1,
            "far": lambda s: (s + 1 if s % 2 else s - 1) % n_space,
        }[tile]
        route = []
        for t in range(n_tm):
            for s in range(n_space):
                other = (t // 2 ^ y) * 2 + (t % 2 ^ core)
                route.append((other * n_space + partner(s), t * n_space + s))
        return lax.ppermute(block, ("tm", "space"), route)

    def steps(
        state, obs_start, foot_weight, obs_slot, obs_frac, live_count, obs_values, jacobian, inv_var
    ):
        own = state[0]
        cols, levels = own.shape
        half = cols // 2
        width = 2 * cols
        chan = jacobian.shape[1]
        obs = obs_start.shape[0]

        def flat(vector):
            return vector.reshape(1, -1)

        (first,) = call(first_kernel, [((8, 128), F32)], flops=FIRST_FLOPS)
        full, near, far, info = call(
            functools.partial(enter_kernel, n_space),
            [
                ((chan, cols), BF16),
                ((chan, half), BF16),
                ((chan, half), BF16),
                ((16, obs), F32),
            ],
            first,
            own.T,
            jacobian,
            flat(obs_start),
            foot_weight.T,
            flat(obs_slot),
            flat(obs_frac),
        )
        near, far = swap(near, tile="near"), swap(far, tile="far")
        infos = [info] + [swap(info, y=j) for j in range(1, lanes)]
        (wide,) = call(widen_kernel, [((chan, width), BF16)], full, near, far)
        other = swap(wide, core=1)
        mats = [None] * lanes
        (mats[2],) = call(footprint, [((width, obs), BF16)], infos[2])

        def gather(which):
            outs = call(
                functools.partial(build_gather_kernel, len(which)),
                [((width, obs), BF16)] * len(which) + [((chan, obs), BF16)] * len(which),
                wide,
                other,
                *[infos[j] for j in which],
            )
            for index, j in enumerate(which):
                mats[j] = outs[index]
            return outs[len(which) :]

        (far,) = call(gather_kernel, [((chan, obs), BF16)], wide, other, infos[2], mats[2])
        parts = [None] * lanes
        parts[2] = swap(far, y=2)
        for j in SWAP_ORDER[1:]:
            (part,) = gather([j])
            parts[j] = swap(part, y=j)
        (parts[0],) = gather([0])
        values, scale = call(
            values_kernel,
            [((chan, obs), F32), ((chan, chan), F32)],
            obs_values,
            flat(inv_var),
            specs=[HBM, VMEM],
            scratch=[pltpu.VMEM((obs, chan), F32), pltpu.SemaphoreType.DMA],
        )
        gaps, scaled = call(
            functools.partial(depart_kernel, lanes),
            [((chan, obs), F32), ((chan, obs), BF16)],
            live_count,
            *parts,
            values,
            scale,
            specs=[SMEM] + [VMEM] * (lanes + 2),
        )
        all_scaled = [scaled] + [swap(scaled, y=j) for j in range(1, lanes)]
        (acc,) = call(spread_first_kernel, [((2 * chan, width), F32)], info, scaled, mats[0])
        (departures,) = call(turn_kernel, [((obs, chan), F32)], gaps)
        *early, last = LAND_ORDER
        for j in early:
            (acc,) = call(
                spread_next_kernel,
                [((2 * chan, width), F32)],
                acc,
                infos[j],
                all_scaled[j],
                mats[j],
            )
        rest = (acc, infos[last], all_scaled[last], mats[last])
        (give,) = call(spread_give_kernel, [((chan, width), BF16)], *rest)
        give = swap(give, core=1)
        (mine,) = call(spread_keep_kernel, [((chan, width), F32)], *rest)
        mid, near, far = call(
            join_kernel, [((chan, cols), F32)] + [((chan, half), BF16)] * 2, mine, give
        )
        pieces = -(-levels // PIECE)
        (adjoint,) = call(
            finish_kernel,
            [((levels, 1, cols), F32)],
            mid,
            swap(near, tile="near"),
            swap(far, tile="far"),
            jacobian,
            out_specs=[HBM],
            scratch=[pltpu.VMEM((levels, 1, cols), F32), pltpu.SemaphoreType.DMA((pieces,))],
        )
        return (departures, jnp.transpose(adjoint, (1, 2, 0)))

    return steps


def solution(mesh):
    return jax.shard_map(
        make_body(mesh.shape["tm"], mesh.shape["space"]),
        mesh=mesh,
        in_specs=(
            P("tm", "space", None),
            P(("tm", "space")),
            P(("tm", "space"), None),
            P(("tm", "space")),
            P(("tm", "space")),
            P("tm", "space"),
            P(("tm", "space"), None),
            P(),
            P(),
        ),
        out_specs=(P(("tm", "space"), None), P("tm", "space", None)),
        check_vma=False,
    )
```

```python
import functools

import jax
import jax.numpy as jnp
from jax import lax
from jax.experimental import pallas as pl
from jax.experimental.pallas import tpu as pltpu
from jax.sharding import PartitionSpec as P


F32 = jnp.float32
BF16 = jnp.bfloat16
GROUP = 16
SWAP_ORDER = (2, 3, 1)
FIRST_FLOPS = 1 << 34


VMEM = pl.BlockSpec(memory_space=pltpu.VMEM)
SMEM = pl.BlockSpec(memory_space=pltpu.SMEM)
HBM = pl.BlockSpec(memory_space=pltpu.HBM)


def held_slots():
    turn = lax.axis_index("tm")
    return turn.astype(F32), (turn ^ 1).astype(F32)


def even_tile():
    return lax.axis_index("space") % 2 == 0


def put_rims(near, far, left, right):
    @pl.when(even_tile())
    def _():
        near[...] = right
        far[...] = left

    @pl.when(jnp.logical_not(even_tile()))
    def _():
        near[...] = left
        far[...] = right


def first_kernel(out):
    out[...] = jnp.zeros_like(out)


def enter_kernel(tiles, first, state, jac, start, weight, slot, frac, full, near, far, info):
    cols = full.shape[1]
    half = cols // 2
    out = lax.dot_general(
        jac[...], state[...], (((0,), (0,)), ((), ())), preferred_element_type=F32
    ).astype(BF16)
    full[...] = out
    put_rims(near, far, out[:, :half], out[:, half:])
    base = lax.axis_index("space") * cols - half
    total = cols * tiles
    local = start[...] - base
    local = jnp.where(local < 0, local + total, local)
    local = jnp.where(local >= total, local - total, local)
    rows = lax.broadcasted_iota(jnp.int32, (8, local.shape[1]), 0)
    extra = jnp.where(rows == 0, local.astype(F32), 0.0)
    extra = jnp.where(rows == 1, slot[...].astype(F32), extra)
    extra = jnp.where(rows == 2, frac[...], extra)
    info[0:8, :] = weight[...].astype(F32)
    info[8:16, :] = extra


def widen_kernel(full, near, far, wide):
    cols = full.shape[1]
    half = cols // 2
    wide[:, half : half + cols] = full[...]

    @pl.when(even_tile())
    def _():
        wide[:, :half] = far[...]
        wide[:, half + cols :] = near[...]

    @pl.when(jnp.logical_not(even_tile()))
    def _():
        wide[:, :half] = near[...]
        wide[:, half + cols :] = far[...]


def footprint(info, mat):
    width, obs = mat.shape
    local = info[8:9, :].astype(jnp.int32)
    low = local & (GROUP - 1)
    high = lax.shift_right_logical(local, 4)
    rows = lax.broadcasted_iota(jnp.int32, (GROUP, obs), 0)
    offset = (rows - low) & (GROUP - 1)
    piece = jnp.zeros((GROUP, obs), F32)
    for k in range(8):
        piece = piece + jnp.where(offset == k, info[k : k + 1, :], 0.0)
    piece = piece.astype(BF16)
    group = (high + jnp.where(rows < low, 1, 0)).astype(F32).astype(BF16)
    zero = jnp.zeros((GROUP, obs), BF16)
    for g in range(width // GROUP):
        mat[g * GROUP : (g + 1) * GROUP, :] = jnp.where(
            group == jnp.full((GROUP, obs), g, BF16), piece, zero
        )


def slot_weight(info, held):
    slot = info[9:10, :]
    frac = info[10:11, :]
    return jnp.where(slot == held, 1.0 - frac, 0.0) + jnp.where(slot + 1.0 == held, frac, 0.0)


def gather_one(field, info, mat, out):
    chan = out.shape[0]
    own_slot, other_slot = held_slots()
    both = jnp.dot(field, mat[...], preferred_element_type=F32)
    first = slot_weight(info, own_slot)
    second = slot_weight(info, other_slot)
    out[...] = (first * both[:chan] + second * both[chan:]).astype(BF16)


def gather_kernel(mine, other, info, mat, out):
    gather_one(jnp.concatenate([mine[...], other[...]], axis=0), info, mat, out)


def build_gather_kernel(n, mine, other, *refs):
    infos, mats, outs = refs[:n], refs[n : 2 * n], refs[2 * n :]
    field = jnp.concatenate([mine[...], other[...]], axis=0)
    for info, mat, out in zip(infos, mats, outs):
        footprint(info, mat)
        gather_one(field, info, mat, out)


def turn_kernel(source, out):
    out[...] = jnp.transpose(source[...])


def values_kernel(source, inv_var, values, scale, held, sem):
    copy = pltpu.make_async_copy(source, held, sem)
    copy.start()
    scale[...] = jnp.transpose(jnp.broadcast_to(inv_var[...], scale.shape))
    copy.wait()
    values[...] = jnp.transpose(held[...])


def depart_kernel(n, count, *refs):
    parts = refs[:n]
    values, scale, gaps, scaled = refs[n:]
    chan, obs = values.shape
    total = parts[0][...].astype(F32)
    for part in parts[1:]:
        total = total + part[...].astype(F32)
    live = lax.broadcasted_iota(jnp.int32, (chan, obs), 1) < count[0, 0]
    gap = jnp.where(live, values[...] - total, 0.0)
    gaps[...] = gap
    scaled[...] = (gap * scale[:, 0:1]).astype(BF16)


def weighted(info, source, slot):
    return (slot_weight(info, slot) * source[...].astype(F32)).astype(BF16)


def spread_rows(rows, mat):
    return lax.dot_general(
        rows, mat[...], (((1,), (1,)), ((), ())), preferred_element_type=F32
    )


def spread_one(info, source, mat):
    rows = [weighted(info, source, slot) for slot in held_slots()]
    return spread_rows(jnp.concatenate(rows, axis=0), mat)


def spread_first_kernel(info, scaled, mat, acc):
    acc[...] = spread_one(info, scaled, mat)


def spread_next_kernel(before, info, scaled, mat, acc):
    acc[...] = before[...] + spread_one(info, scaled, mat)


def spread_last_kernel(before, *refs):
    infos, scaled, mats = refs[:2], refs[2:4], refs[4:6]
    own, give = refs[6:]
    chan = own.shape[0]
    total = before[...]
    for info, source, mat in zip(infos, scaled, mats):
        total = total + spread_one(info, source, mat)
    own[...] = total[:chan]
    give[...] = total[chan:].astype(BF16)


def join_kernel(own, got, mid, near, far):
    cols = mid.shape[1]
    half = cols // 2
    mid[...] = own[:, half : half + cols] + got[:, half : half + cols].astype(F32)
    left = (own[:, :half] + got[:, :half].astype(F32)).astype(BF16)
    right = (own[:, half + cols :] + got[:, half + cols :].astype(F32)).astype(BF16)
    put_rims(near, far, left, right)


def finish_kernel(mid, near, far, jac, out, rows, sems):
    half = near.shape[1]
    levels = jac.shape[0]
    cut = (levels // 2 + 15) // 16 * 16
    even = even_tile()
    first = mid[:, :half] + jnp.where(even, far[...], near[...]).astype(F32)
    last = mid[:, half:] + jnp.where(even, near[...], far[...]).astype(F32)
    total = jnp.concatenate([first, last], axis=1).astype(BF16)
    copies = []
    for index, part in enumerate((slice(0, cut), slice(cut, levels))):
        rows[part, 0, :] = jnp.dot(jac[part, :], total, preferred_element_type=F32)
        copy = pltpu.make_async_copy(rows.at[part], out.at[part], sems.at[index])
        copy.start()
        copies.append(copy)
    for copy in copies:
        copy.wait()


def call(kernel, outs, *args, specs=None, out_specs=None, scratch=(), limit=8 << 20, flops=1 << 20):
    return pl.pallas_call(
        kernel,
        out_shape=[jax.ShapeDtypeStruct(shape, dtype) for shape, dtype in outs],
        in_specs=specs or [VMEM] * len(args),
        out_specs=out_specs or [VMEM] * len(outs),
        scratch_shapes=scratch,
        compiler_params=pltpu.CompilerParams(vmem_limit_bytes=limit),
        cost_estimate=pl.CostEstimate(flops=flops, bytes_accessed=1 << 20, transcendentals=0),
    )(*args)


def make_body(n_tm, n_space):
    lanes = n_tm // 2

    def swap(block, y=0, core=0, tile=None):
        partner = {
            None: lambda s: s,
            "near": lambda s: s ^ 1,
            "far": lambda s: (s + 1 if s % 2 else s - 1) % n_space,
        }[tile]
        route = []
        for t in range(n_tm):
            for s in range(n_space):
                other = (t // 2 ^ y) * 2 + (t % 2 ^ core)
                route.append((other * n_space + partner(s), t * n_space + s))
        return lax.ppermute(block, ("tm", "space"), route)

    def steps(
        state, obs_start, foot_weight, obs_slot, obs_frac, live_count, obs_values, jacobian, inv_var
    ):
        own = state[0]
        cols, levels = own.shape
        half = cols // 2
        width = 2 * cols
        chan = jacobian.shape[1]
        obs = obs_start.shape[0]

        def flat(vector):
            return vector.reshape(1, -1)

        (first,) = call(first_kernel, [((8, 128), F32)], flops=FIRST_FLOPS)
        full, near, far, info = call(
            functools.partial(enter_kernel, n_space),
            [
                ((chan, cols), BF16),
                ((chan, half), BF16),
                ((chan, half), BF16),
                ((16, obs), F32),
            ],
            first,
            own.T,
            jacobian,
            flat(obs_start),
            foot_weight.T,
            flat(obs_slot),
            flat(obs_frac),
        )
        near, far = swap(near, tile="near"), swap(far, tile="far")
        infos = [info] + [swap(info, y=j) for j in range(1, lanes)]
        (wide,) = call(widen_kernel, [((chan, width), BF16)], full, near, far)
        other = swap(wide, core=1)
        mats = [None] * lanes
        (mats[2],) = call(footprint, [((width, obs), BF16)], infos[2])

        def gather(which):
            outs = call(
                functools.partial(build_gather_kernel, len(which)),
                [((width, obs), BF16)] * len(which) + [((chan, obs), BF16)] * len(which),
                wide,
                other,
                *[infos[j] for j in which],
            )
            for index, j in enumerate(which):
                mats[j] = outs[index]
            return outs[len(which) :]

        (far,) = call(gather_kernel, [((chan, obs), BF16)], wide, other, infos[2], mats[2])
        parts = [None] * lanes
        parts[2] = swap(far, y=2)
        for j in SWAP_ORDER[1:]:
            (part,) = gather([j])
            parts[j] = swap(part, y=j)
        (parts[0],) = gather([0])
        values, scale = call(
            values_kernel,
            [((chan, obs), F32), ((chan, chan), F32)],
            obs_values,
            flat(inv_var),
            specs=[HBM, VMEM],
            scratch=[pltpu.VMEM((obs, chan), F32), pltpu.SemaphoreType.DMA],
        )
        gaps, scaled = call(
            functools.partial(depart_kernel, lanes),
            [((chan, obs), F32), ((chan, obs), BF16)],
            live_count,
            *parts,
            values,
            scale,
            specs=[SMEM] + [VMEM] * (lanes + 2),
        )
        all_scaled = [scaled] + [swap(scaled, y=j) for j in range(1, lanes)]
        (acc,) = call(spread_first_kernel, [((2 * chan, width), F32)], info, scaled, mats[0])
        (departures,) = call(turn_kernel, [((obs, chan), F32)], gaps)
        (acc,) = call(
            spread_next_kernel, [((2 * chan, width), F32)], acc, infos[2], all_scaled[2], mats[2]
        )
        mine, give = call(
            spread_last_kernel,
            [((chan, width), F32), ((chan, width), BF16)],
            acc,
            *[infos[j] for j in (1, 3)],
            *[all_scaled[j] for j in (1, 3)],
            *[mats[j] for j in (1, 3)],
        )
        give = swap(give, core=1)
        mid, near, far = call(
            join_kernel, [((chan, cols), F32)] + [((chan, half), BF16)] * 2, mine, give
        )
        (adjoint,) = call(
            finish_kernel,
            [((levels, 1, cols), F32)],
            mid,
            swap(near, tile="near"),
            swap(far, tile="far"),
            jacobian,
            out_specs=[HBM],
            scratch=[pltpu.VMEM((levels, 1, cols), F32), pltpu.SemaphoreType.DMA((2,))],
        )
        return (departures, jnp.transpose(adjoint, (1, 2, 0)))

    return steps


def solution(mesh):
    return jax.shard_map(
        make_body(mesh.shape["tm"], mesh.shape["space"]),
        mesh=mesh,
        in_specs=(
            P("tm", "space", None),
            P(("tm", "space")),
            P(("tm", "space"), None),
            P(("tm", "space")),
            P(("tm", "space")),
            P("tm", "space"),
            P(("tm", "space"), None),
            P(),
            P(),
        ),
        out_specs=(P(("tm", "space"), None), P("tm", "space", None)),
        check_vma=False,
    )
```
